128 devices in a mesh: edp: 2 (over y_hi), ep: 64 (over y_lo, z, x, core).
Axes of the slice: x: 4, y: 4 (y_hi: 2, y_lo: 2; y = y_hi * 2 + y_lo), z: 4, core: 2. Of those that a mesh axis runs over, the one named last changes fastest.
Arguments:
- tokens: bfloat16 [16384, 2048], P(('edp', 'ep')), may hold values from -6 to 6
- routes: int32 [16384, 8], P(('edp', 'ep')), may hold values from 0 to 63, all different within a row; in each aligned block of 128 rows (0 to 127, 128 to 255, ...) at most 24 rows name the same one
- gate_weights: float32 [16384, 8], P(('edp', 'ep')), may hold values from 0.05 to 0.5
- w_gate: bfloat16 [64, 2048, 768], P('ep'), may hold values from -0.125 to 0.125
- w_up: bfloat16 [64, 2048, 768], P('ep'), may hold values from -0.125 to 0.125
- w_down: bfloat16 [64, 768, 2048], P('ep'), may hold values from -0.21875 to 0.21875
- saved_inputs: bfloat16 [64, 512, 2048], P('ep', 'edp'), may hold values from -6 to 6
- saved_cotangent: bfloat16 [64, 512, 2048], P('ep', 'edp'), may hold values from -0.59765625 to 0.59765625
Outputs:
- mixed: bfloat16 [16384, 2048], P(('edp', 'ep'))
- grad_gate: float32 [64, 2048, 768], P('ep', 'edp')
- grad_up: float32 [64, 2048, 768], P('ep', 'edp')
- grad_down: float32 [64, 768, 2048], P('ep', 'edp')
The draws below stay inside these ranges and needn't reach their ends.
Inputs may be any that keep to these rules, and one draw needn't show every extreme that they name: `routes`: each token names 8 different experts. In each aligned block of 128 tokens (the tokens of one device) no expert is named more than 24 times, a bound that some block reaches in every draw.
All inputs are finite; a program needn't handle non-finite values.
Results may differ from the reference program's by a relative error of at most 0.006.
Values may be sent and summed in bfloat16 or wider, within the bound.
A program may use at most 128 MiB of HBM per device.

```python
import math
import jax
import jax.numpy as jnp
import numpy as np
from jax import lax

D = 2048
FF = 768
TOP = 8
TOK_DEV = 128
ROWS_BWD = 256
EXPERTS = 64
CAP = 24
TOKENS = 16384
BWD_ROWS = 512
N_EDP = 2


def levels(rng, dims, split, smallest, largest):
    gain, own = 1.0, jax.random.fold_in(rng, 6)
    for axis_at, blocks in split:
        steps = jnp.exp(jax.random.uniform(jax.random.fold_in(own, axis_at), (blocks,), jnp.float32, smallest / len(split), largest / len(split)))
        gain = gain * jnp.repeat(steps, dims[axis_at] // blocks).reshape([-1 if axis == axis_at else 1 for axis in range(len(dims))])
    return gain


def routed_block(stream_key, own, number, rows, number_of, top, reach, lean):
    order = jax.random.permutation(stream_key, number_of)
    packed, ordinary = portions_of(number_of, rows * top, reach, lean, True), portions_of(number_of, rows * top, reach, lean, False)
    places = jnp.arange(number_of)

    def named(tallies, offset_by):
        used = int((tallies > 0).sum())
        fixed = max(1, used // 4)
        shifted = fixed + (places - fixed + offset_by * (used - fixed)) % max(1, number_of - fixed)
        return jnp.zeros((number_of,), jnp.int32).at[order[jnp.where(places < fixed, places, shifted)]].set(jnp.asarray(tallies, jnp.int32))

    tallies = jnp.where(number % 4 == 0, named(packed, number // 4), named(ordinary, number - number // 4 - 1))
    mixed = jax.random.permutation(jax.random.fold_in(own, 3), number_of)
    source_of, receiver = mixed[0:number_of // 2 * 2:2], mixed[1:number_of // 2 * 2:2]
    margin = jnp.minimum(tallies[source_of] - 1, reach - tallies[receiver]) // 2
    margin = jnp.where((source_of == order[0]) | (receiver == order[0]) | (tallies[receiver] == 0), 0, jnp.maximum(margin, 0))
    shifted = jax.random.randint(jax.random.fold_in(own, 4), (number_of // 2,), 0, 1 << 20) % (margin + 1)
    tallies = tallies.at[source_of].add(-shifted).at[receiver].add(shifted)
    items = jnp.searchsorted(jnp.cumsum(tallies), jnp.arange(rows * top), side="right").astype(jnp.int32)
    listing = items.reshape(top, rows).T
    listing = listing[jax.random.permutation(jax.random.fold_in(own, 1), rows)]
    offset_by = jax.random.randint(jax.random.fold_in(own, 2), (rows, 1), 0, top)
    return jnp.take_along_axis(listing, (jnp.arange(top)[None, :] + offset_by) % top, axis=1)


def portions_of(amount, total, limit, slope, full):
    weights = [(1 << 20) // math.isqrt(rank ** slope) + 1 for rank in range(1, amount + 1)]
    largest = limit if full else min(limit, max(-(-total // amount), total * weights[0] // sum(weights)))
    least = 1 if total - largest >= amount - 1 else 0
    holding, surplus = [largest] + [least] * (amount - 1), total - largest - least * (amount - 1)
    while surplus > 0:
        movable = [i for i in range(1, amount) if holding[i] < largest] or [i for i in range(1, amount) if holding[i] < limit]
        mass, budget = sum([weights[i] for i in movable]), surplus
        for i in movable:
            addition = min(limit - holding[i], max(1, budget * weights[i] // mass), surplus)
            holding[i] = holding[i] + addition
            surplus = surplus - addition
    return np.array(holding)


def noise(own_key, extent, scale, most, shards=(), kind=jnp.bfloat16):
    drawn = jax.random.normal(own_key, extent, jnp.float32) * scale
    if len(shards) > 0:
        drawn = levels(own_key, extent, shards, -0.22, 0.18) * drawn
    return jnp.clip(drawn, min=-most, max=most).astype(kind)


def setup_inputs(seed: int = 0) -> dict:
    streams_of = jax.random.split(jax.random.key(seed), 9)
    tokens = noise(streams_of[0], (TOKENS, D), 1.0, 6.0, ((0, 128),))
    routes_keys = jax.random.split(jax.random.fold_in(streams_of[1], 1), TOKENS // TOK_DEV)
    routes_turns = jax.random.permutation(jax.random.fold_in(streams_of[1], 3), TOKENS // TOK_DEV)
    routes = jax.vmap(lambda own, number: routed_block(jax.random.fold_in(streams_of[1], 2), own, number, TOK_DEV, EXPERTS, TOP, CAP, 2))(routes_keys, routes_turns).reshape((TOKENS, TOP))
    gate_weights = jnp.clip(jnp.exp(math.log(0.5) - 2.3025851 * jax.random.uniform(streams_of[2], (TOKENS, TOP), jnp.float32) ** levels(streams_of[2], (TOKENS, TOP), ((0, 128),), -0.2, 0.2)), 0.05, 0.5)
    w_gate = noise(streams_of[3], (EXPERTS, D, FF), D ** -0.5, 0.125, ((0, 64),))
    w_up = noise(streams_of[4], (EXPERTS, D, FF), D ** -0.5, 0.125, ((0, 64),))
    w_down = noise(streams_of[5], (EXPERTS, FF, D), FF ** -0.5, 0.21875, ((0, 64),))
    saved_inputs = noise(streams_of[6], (EXPERTS, BWD_ROWS, D), 1.0, 6.0, ((0, 64), (1, 2)))
    saved_cotangent = noise(streams_of[7], (EXPERTS, BWD_ROWS, D), 0.1, 0.59765625, ((0, 64), (1, 2)))
    return {"tokens": tokens, "routes": routes, "gate_weights": gate_weights, "w_gate": w_gate, "w_up": w_up, "w_down": w_down, "saved_inputs": saved_inputs, "saved_cotangent": saved_cotangent}


def expert_mlp(row_data, w_gate, w_up, w_down):
    gate_pre = jnp.dot(row_data, w_gate, preferred_element_type=jnp.float32)
    up_pre = jnp.dot(row_data, w_up, preferred_element_type=jnp.float32)
    hidden = (jax.nn.silu(gate_pre) * up_pre).astype(jnp.bfloat16)
    return jnp.dot(hidden, w_down, preferred_element_type=jnp.float32).astype(jnp.bfloat16)


def expert_grads(inputs, cotangent, w_gate, w_up, w_down):
    gate_pre = jnp.dot(inputs, w_gate, preferred_element_type=jnp.float32)
    up_pre = jnp.dot(inputs, w_up, preferred_element_type=jnp.float32)
    activated = jax.nn.silu(gate_pre)
    hidden = (activated * up_pre).astype(jnp.bfloat16)
    d_hidden = jnp.dot(cotangent, w_down.T, preferred_element_type=jnp.float32)
    sigmoid_gate = jax.nn.sigmoid(gate_pre)
    d_gate = (d_hidden * up_pre * sigmoid_gate * (1.0 + gate_pre * (1.0 - sigmoid_gate))).astype(jnp.bfloat16)
    d_up = (d_hidden * activated).astype(jnp.bfloat16)
    return hidden, d_gate, d_up


def rounded(value):
    return lax.optimization_barrier(value.astype(jnp.bfloat16)).astype(jnp.float32)


def reference(tokens, routes, gate_weights, w_gate, w_up, w_down, saved_inputs, saved_cotangent):
    blocks = TOKENS // TOK_DEV
    route_blocks = routes.reshape(blocks, TOK_DEV * TOP)
    one_hot = (route_blocks[:, :, None] == jnp.arange(EXPERTS, dtype=jnp.int32)[None, None, :]).astype(jnp.int32)
    running = jnp.cumsum(one_hot, axis=1) - 1
    slot_index = jnp.sum(running * one_hot, axis=2)
    position = jnp.arange(blocks, dtype=jnp.int32)[:, None] * CAP + slot_index
    token_id = (jnp.arange(TOKENS * TOP, dtype=jnp.int32) // TOP).astype(jnp.int32)
    row_count = blocks * CAP
    row_table = jnp.full((EXPERTS, row_count), TOKENS, jnp.int32)
    row_table = row_table.at[route_blocks.reshape(-1), position.reshape(-1)].set(token_id)
    weight_table = jnp.zeros((EXPERTS, row_count), jnp.float32)
    weight_table = weight_table.at[route_blocks.reshape(-1), position.reshape(-1)].set(gate_weights.reshape(-1))
    padded = jnp.concatenate([tokens, jnp.zeros((1, D), tokens.dtype)], axis=0)

    def one_expert(accum_rows, expert_data):
        row_ids, weights, gate_mat, up_mat, down_mat = expert_data
        output = expert_mlp(padded[row_ids], gate_mat, up_mat, down_mat)
        accum_rows = accum_rows.at[row_ids].add(weights[:, None] * output.astype(jnp.float32))
        return accum_rows, None

    summed, unused = lax.scan(one_expert, jnp.zeros((TOKENS + 1, D), jnp.float32),
                              (row_table, weight_table, w_gate, w_up, w_down))
    mixed = summed[:TOKENS].astype(jnp.bfloat16)

    def expert_backward(expert_data):
        inputs_all, cotangent_all, gate_mat, up_mat, down_mat = expert_data
        grad_g = jnp.zeros((D, FF), jnp.float32)
        grad_u = jnp.zeros((D, FF), jnp.float32)
        grad_d = jnp.zeros((FF, D), jnp.float32)
        for replica in range(N_EDP):
            inputs = inputs_all[replica * ROWS_BWD:(replica + 1) * ROWS_BWD]
            cotangent = cotangent_all[replica * ROWS_BWD:(replica + 1) * ROWS_BWD]
            hidden, d_gate, d_up = expert_grads(inputs, cotangent, gate_mat, up_mat, down_mat)
            grad_g = grad_g + rounded(jnp.dot(inputs.T, d_gate, preferred_element_type=jnp.float32))
            grad_u = grad_u + rounded(jnp.dot(inputs.T, d_up, preferred_element_type=jnp.float32))
            grad_d = grad_d + rounded(jnp.dot(hidden.T, cotangent, preferred_element_type=jnp.float32))
        return grad_g, grad_u, grad_d

    grad_gate, grad_up, grad_down = lax.map(expert_backward, (saved_inputs, saved_cotangent, w_gate, w_up, w_down))
    return mixed, grad_gate, grad_up, grad_down
```

```python
import jax
import jax.numpy as jnp
from jax import lax
from jax.sharding import PartitionSpec as P

CAP = 24


def expert_mlp(row_data, w_gate, w_up, w_down):
    gate_pre = jnp.dot(row_data, w_gate, preferred_element_type=jnp.float32)
    up_pre = jnp.dot(row_data, w_up, preferred_element_type=jnp.float32)
    hidden = (jax.nn.silu(gate_pre) * up_pre).astype(jnp.bfloat16)
    return jnp.dot(hidden, w_down, preferred_element_type=jnp.float32).astype(jnp.bfloat16)


def expert_grads(inputs, cotangent, w_gate, w_up, w_down):
    gate_pre = jnp.dot(inputs, w_gate, preferred_element_type=jnp.float32)
    up_pre = jnp.dot(inputs, w_up, preferred_element_type=jnp.float32)
    activated = jax.nn.silu(gate_pre)
    hidden = (activated * up_pre).astype(jnp.bfloat16)
    d_hidden = jnp.einsum("rd,fd->rf", cotangent, w_down, preferred_element_type=jnp.float32)
    sigmoid_gate = jax.nn.sigmoid(gate_pre)
    d_gate = (d_hidden * up_pre * sigmoid_gate * (1.0 + gate_pre * (1.0 - sigmoid_gate))).astype(
        jnp.bfloat16
    )
    d_up = (d_hidden * activated).astype(jnp.bfloat16)
    return (hidden, d_gate, d_up)


def rounded(value):
    return lax.optimization_barrier(value.astype(jnp.bfloat16)).astype(jnp.float32)


def slot_tables(routes, gate_weights, experts):
    rows = routes.shape[0]
    chosen = routes[:, :, None] == jnp.arange(experts, dtype=jnp.int32)[None, None, :]
    named = jnp.any(chosen, axis=1)
    weight = jnp.sum(jnp.where(chosen, gate_weights[:, :, None], 0.0), axis=1)
    earlier = (jnp.arange(rows)[:, None] > jnp.arange(rows)[None, :]).astype(jnp.bfloat16)
    count = jnp.dot(earlier, named.astype(jnp.bfloat16), preferred_element_type=jnp.float32)
    slot = jnp.where(named, count, -1.0)
    return slot, weight


def shards(tokens, routes, gate_weights, w_gate, w_up, w_down, saved_inputs, saved_cotangent):
    experts = lax.axis_size("ep")
    tok_rows, width = tokens.shape
    slot, weight = slot_tables(routes, gate_weights, experts)
    places = jnp.arange(CAP, dtype=jnp.float32)
    pick = (slot.T[:, None, :] == places[None, :, None]).astype(jnp.bfloat16)
    send_buffer = jnp.dot(pick.reshape(experts * CAP, tok_rows), tokens,
                          preferred_element_type=jnp.float32).astype(jnp.bfloat16)
    send_buffer = send_buffer.reshape(experts, CAP, width)
    gate_mat, up_mat, down_mat = (w_gate[0], w_up[0], w_down[0])
    swap = [(0, 1), (1, 0)]
    peer_inputs = lax.ppermute(saved_inputs[0], "edp", swap)
    peer_cotangent = lax.ppermute(saved_cotangent[0], "edp", swap)
    received = lax.all_to_all(send_buffer, "ep", split_axis=0, concat_axis=0, tiled=True)
    output = expert_mlp(received.reshape(-1, width), gate_mat, up_mat, down_mat)
    returned = lax.all_to_all(
        output.reshape(received.shape), "ep", split_axis=0, concat_axis=0, tiled=True
    ).reshape(experts * CAP, width)
    mix = jnp.where(slot[:, :, None] == places[None, None, :], weight[:, :, None], 0.0)
    mix = mix.reshape(tok_rows, experts * CAP)
    high = mix.astype(jnp.bfloat16)
    low = (mix - high.astype(jnp.float32)).astype(jnp.bfloat16)
    combined = (
        jnp.dot(high, returned, preferred_element_type=jnp.float32)
        + jnp.dot(low, returned, preferred_element_type=jnp.float32)
    ).astype(jnp.bfloat16)
    replicas = lax.axis_size("edp")
    own_index = lax.axis_index("edp")
    half_width = width // replicas
    half_hidden = gate_mat.shape[1] // replicas
    sums = None
    for inputs, cotangent in ((saved_inputs[0], saved_cotangent[0]), (peer_inputs, peer_cotangent)):
        hidden, d_gate, d_up = expert_grads(inputs, cotangent, gate_mat, up_mat, down_mat)
        in_cols = lax.dynamic_slice_in_dim(inputs, own_index * half_width, half_width, 1)
        hidden_cols = lax.dynamic_slice_in_dim(hidden, own_index * half_hidden, half_hidden, 1)
        parts = [
            rounded(jnp.einsum("rd,rf->df", in_cols, d_gate, preferred_element_type=jnp.float32)),
            rounded(jnp.einsum("rd,rf->df", in_cols, d_up, preferred_element_type=jnp.float32)),
            rounded(jnp.einsum("rf,rd->fd", hidden_cols, cotangent, preferred_element_type=jnp.float32)),
        ]
        sums = parts if sums is None else [a + b for a, b in zip(sums, parts)]
    return (combined, sums[0][None], sums[1][None], sums[2][None])


def solution(mesh):
    return jax.shard_map(
        shards,
        mesh=mesh,
        in_specs=(
            P(("edp", "ep"), None),
            P(("edp", "ep"), None),
            P(("edp", "ep"), None),
            P("ep", None, None),
            P("ep", None, None),
            P("ep", None, None),
            P("ep", "edp", None),
            P("ep", "edp", None),
        ),
        out_specs=(
            P(("edp", "ep"), None),
            P("ep", "edp", None),
            P("ep", "edp", None),
            P("ep", "edp", None),
        ),
        check_vma=False,
    )
```

```python
import jax
import jax.numpy as jnp
from jax import lax
from jax.experimental import pallas as pl
from jax.experimental.pallas import tpu as pltpu
from jax.sharding import PartitionSpec as P

CAP = 24
SIDE = 4
TARGETS = 8
PAIR = 2 * CAP
CHUNK = TARGETS * PAIR
TILE = 256
ORDER = (0, 1, 3, 2)
BF = jnp.bfloat16
F32 = jnp.float32


def dot(a, b, dims=((1,), (0,))):
    return lax.dot_general(a, b, (dims, ((), ())), preferred_element_type=F32)


def tile(n, size=TILE):
    return pl.ds(pl.multiple_of(n * size, size), size)


def loop(count, body):
    def step(n, carry):
        body(n)
        return carry

    lax.fori_loop(0, count, step, 0)


def kernel(
    routes, gates, tokens, w_gate, w_up, w_down, saved_x, saved_y,
    mixed, grad_gate, grad_up, grad_down,
    wg, wu, wd, blocks, aux, aux32, hot, hot_lhs, mix_lhs, packed, recv, back, part, gathered,
    y_send, y_recv, total, xs, ys, hid, dgs, dus, hbuf, stage_a, stage_b,
    load_sem, y_s, y_r, a_s, a_r, b_s, b_r, rb_s, rb_r, ra_s, ra_r, ry_s, ry_r, e_s, e_r, out_sem, mix_sem,
):
    width = blocks.shape[-1]
    rows = blocks.shape[1] // 2
    hidden_width = wg.shape[1]
    half_width = width // 2
    half_hidden = hidden_width // 2
    tiles = width // TILE

    me = lax.axis_index("ep")
    replica = lax.axis_index("edp")
    core = lax.rem(me, 2)
    x = lax.rem(me // 2, SIDE)
    z = lax.rem(me // (2 * SIDE), SIDE)
    y = me // (2 * SIDE * SIDE)
    a = z * (1 - core) + x * core
    b = x * (1 - core) + z * core

    def place(yy, aa, bb, cc):
        aa = lax.rem(aa, SIDE)
        bb = lax.rem(bb, SIDE)
        zz = aa * (1 - core) + bb * core
        xx = bb * (1 - core) + aa * core
        return ((yy * SIDE + zz) * SIDE + xx) * 2 + cc

    def at(index):
        return (replica, index)

    y_peer = at(place(1 - y, a, b, core))
    edp_peer = (1 - replica, me)

    def forward_to(t):
        f, g = t // 2, t % 2
        return place(y, a, b + f, core if g == 0 else 1 - core)

    def forwarder(t):
        f, g = t // 2, t % 2
        if g == 0:
            return place(y, a, b + SIDE - f, core)
        return place(y, a + SIDE - f, b, 1 - core)

    loads = [
        pltpu.make_async_copy(tokens, blocks.at[0, 0:rows], load_sem.at[0]),
        pltpu.make_async_copy(saved_x.at[0], xs.at[0], load_sem.at[1]),
        pltpu.make_async_copy(saved_y.at[0], ys.at[0], load_sem.at[2]),
        pltpu.make_async_copy(w_gate.at[0], wg, load_sem.at[3]),
        pltpu.make_async_copy(w_up.at[0], wu, load_sem.at[4]),
        pltpu.make_async_copy(w_down.at[0], wd, load_sem.at[5]),
    ]
    for copy in loads:
        copy.start()

    barrier = pltpu.get_barrier_semaphore()
    peers = [y_peer, edp_peer]
    peers += [at(place(y, a + d, b, core)) for d in range(1, SIDE)]
    peers += [at(place(y, a, b + d, core)) for d in range(1, SIDE)]
    peers += [at(place(y, a, b + d, 1 - core)) for d in range(SIDE)]
    peers += [at(place(y, a + d, b, 1 - core)) for d in range(1, SIDE)]
    for peer in peers:
        pl.semaphore_signal(barrier, inc=1, device_id=peer, device_id_type=pl.DeviceIdType.MESH)

    experts = TARGETS * TARGETS
    names = lax.broadcasted_iota(jnp.int32, (experts, rows), 0)
    named = jnp.zeros((experts, rows), F32)
    weight = jnp.zeros((experts, rows), F32)
    for k in range(routes.shape[0]):
        match = names == routes[k : k + 1, :]
        named = named + jnp.where(match, 1.0, 0.0)
        weight = weight + jnp.where(match, gates[k : k + 1, :], 0.0)
    earlier = (
        lax.broadcasted_iota(jnp.int32, (rows, rows), 0)
        < lax.broadcasted_iota(jnp.int32, (rows, rows), 1)
    )
    earlier = jnp.where(earlier, 1.0, 0.0).astype(BF)
    count = dot(named.astype(BF), earlier)
    aux[0, 0, 0:experts, :] = jnp.where(named > 0.5, count, -1.0).astype(BF)
    aux[0, 0, experts : 2 * experts, :] = weight.astype(BF)
    hot[...] = jnp.zeros_like(hot)

    pl.semaphore_wait(barrier, len(peers))
    loads[0].wait()

    def remote(src, dst, send, receive, peer):
        return pltpu.make_async_remote_copy(
            src_ref=src, dst_ref=dst, send_sem=send, recv_sem=receive,
            device_id=peer, device_id_type=pl.DeviceIdType.MESH,
        )

    own, other = pl.ds(0, rows), pl.ds(rows, rows)
    y_copies = [
        remote(aux.at[0, 0], aux.at[0, 1], y_s.at[0], y_r.at[0], y_peer),
        remote(blocks.at[0, own], blocks.at[0, other], y_s.at[1], y_r.at[1], y_peer),
    ]
    for copy in y_copies:
        copy.start()
    a_copies = {}
    for d in (1, 3, 2):
        peer = at(place(y, a + d, b, core))
        for dy, where in ((0, own), (1, other)):
            a_copies[d, dy] = [
                remote(aux.at[0, dy], aux.at[d, dy], a_s.at[d - 1, 2 * dy], a_r.at[d - 1, 2 * dy], peer),
                remote(blocks.at[0, where], blocks.at[d, where], a_s.at[d - 1, 2 * dy + 1],
                       a_r.at[d - 1, 2 * dy + 1], peer),
            ]
    for d in (1, 3, 2):
        for copy in a_copies[d, 0]:
            copy.start()
    loads[1].wait()
    loads[2].wait()
    e_copies = [
        remote(xs.at[0], xs.at[1], e_s.at[0], e_r.at[0], edp_peer),
        remote(ys.at[0], ys.at[1], e_s.at[1], e_r.at[1], edp_peer),
    ]
    for copy in e_copies:
        copy.start()

    def backward(r):
        def body(n):
            cols = tile(n)
            g = dot(xs[r], wg[:, cols])
            u = dot(xs[r], wu[:, cols])
            dh = dot(ys[r], wd[cols, :], ((1,), (1,)))
            s = jax.nn.sigmoid(g)
            act = g * s
            hid[r, :, cols] = (act * u).astype(BF)
            dgs[r, :, cols] = (dh * u * s * (1.0 + g * (1.0 - s))).astype(BF)
            dus[r, :, cols] = (dh * act).astype(BF)

        loop(hidden_width // TILE, body)

    def fill_hot(d, weighted):
        slots = lax.broadcasted_iota(jnp.int32, (CAP, rows), 0).astype(F32)
        for dy in range(2):
            aux32[dy] = aux[d, dy].astype(F32)
        for t in range(TARGETS):
            e = forward_to(t)
            for dy in range(2):
                hit = aux32[dy, pl.ds(e, 1), :] == slots
                value = aux32[dy, pl.ds(e + experts, 1), :] if weighted else 1.0
                at_row = PAIR * t + CAP * dy
                hot[at_row : at_row + CAP, rows * dy : rows * dy + rows] = jnp.where(hit, value, 0.0)

    def b_copy(d, t):
        span = pl.ds(PAIR * t, PAIR)
        return remote(packed.at[d, span], recv.at[d, span], b_s.at[d, t], b_r.at[d, t], at(forward_to(t)))

    def rb_copy(d, t):
        span = pl.ds(PAIR * t, PAIR)
        return remote(recv.at[d, span], back.at[d, span], rb_s.at[d, t], rb_r.at[d, t], at(forwarder(t)))

    def pack(d):
        fill_hot(d, False)
        hot_lhs[...] = hot[...].astype(BF)

        def body(n):
            cols = tile(n)
            rows_out = dot(hot_lhs[...], blocks[d, :, cols]).astype(BF)
            packed[d, :, cols] = rows_out
            recv[d, 0:PAIR, cols] = rows_out[0:PAIR]

        loop(tiles, body)
        for t in range(1, TARGETS):
            b_copy(d, t).start()

    def mlp(d):
        for t in range(1, TARGETS):
            b_copy(d, t).wait_recv()

        def up(n):
            cols = tile(n)
            g = dot(recv[d], wg[:, cols])
            u = dot(recv[d], wu[:, cols])
            hbuf[:, cols] = (g * jax.nn.sigmoid(g) * u).astype(BF)

        loop(hidden_width // TILE, up)

        def down(n):
            cols = tile(n)
            out = dot(hbuf[...], wd[:, cols]).astype(BF)
            recv[d, :, cols] = out
            back[d, 0:PAIR, cols] = out[0:PAIR]

        loop(tiles, down)
        for t in range(1, TARGETS):
            rb_copy(d, t).start()

    def ra_copy(d, dy):
        span = pl.ds(rows * dy, rows)
        return remote(part.at[d, span], gathered.at[d - 1, span], ra_s.at[d - 1, dy], ra_r.at[d - 1, dy],
                      at(place(y, a + SIDE - d, b, core)))

    def combine(d):
        fill_hot(d, True)
        mix_lhs[...] = hot[...].T.astype(BF)
        for t in range(1, TARGETS):
            rb_copy(d, t).wait_recv()

        def body(n):
            cols = tile(n)
            part[d, :, cols] = dot(mix_lhs[...], back[d, :, cols]).astype(BF)

        loop(tiles, body)
        if d > 0:
            for dy in (1, 0):
                ra_copy(d, dy).start()

    def out_copies(kind, n):
        slot = lax.rem(n, 2)
        if kind == 2:
            return pltpu.make_async_copy(stage_b.at[slot], grad_down.at[0, :, tile(n, stage_b.shape[2])],
                                         out_sem.at[2, slot])
        ref = grad_gate if kind == 0 else grad_up
        return pltpu.make_async_copy(stage_a.at[kind, slot], ref.at[0, tile(n)], out_sem.at[kind, slot])

    def weight_grads():
        def body(n):
            @pl.when(n >= 2)
            def _():
                for kind in range(2):
                    out_copies(kind, n - 2).wait()

            cols = pl.ds(pl.multiple_of(replica * half_width + n * TILE, TILE), TILE)
            slot = lax.rem(n, 2)
            for kind, source in ((0, dgs), (1, dus)):
                sums = [dot(xs[r, :, cols], source[r], ((0,), (0,))).astype(BF).astype(F32) for r in range(2)]
                stage_a[kind, slot] = sums[0] + sums[1]
                out_copies(kind, n).start()

        count = half_width // TILE
        loop(count, body)
        size = stage_b.shape[2]

        def down(n):
            @pl.when(n >= 2)
            def _():
                out_copies(2, n - 2).wait()

            own_cols = pl.ds(pl.multiple_of(replica * half_hidden, 128), half_hidden)
            slot = lax.rem(n, 2)
            sums = [
                dot(hid[r, :, own_cols], ys[r, :, tile(n, size)], ((0,), (0,))).astype(BF).astype(F32)
                for r in range(2)
            ]
            stage_b[slot] = sums[0] + sums[1]
            out_copies(2, n).start()

        loop(width // size, down)
        for n in (count - 2, count - 1):
            for kind in range(2):
                out_copies(kind, n).wait()
        for n in (width // size - 2, width // size - 1):
            out_copies(2, n).wait()

    for copy in loads[3:]:
        copy.wait()
    backward(0)
    for copy in y_copies:
        copy.wait_recv()
    for d in (1, 3, 2):
        for copy in a_copies[d, 1]:
            copy.start()
    pack(0)
    for d in (1, 3):
        for dy in range(2):
            for copy in a_copies[d, dy]:
                copy.wait_recv()
        pack(d)
    mlp(0)
    for dy in range(2):
        for copy in a_copies[2, dy]:
            copy.wait_recv()
    pack(2)
    mlp(1)
    mlp(3)
    mlp(2)
    for copy in e_copies:
        copy.wait_recv()
    backward(1)
    combine(0)
    combine(1)
    combine(3)
    weight_grads()
    combine(2)
    for d in range(1, SIDE):
        ra_copy(d, 1).wait_recv()

    def sums(dy):
        span = pl.ds(rows * dy, rows)

        def body(n):
            cols = tile(n)
            value = part[0, span, cols].astype(F32)
            for d in range(1, SIDE):
                value = value + gathered[d - 1, span, cols].astype(F32)
            if dy == 1:
                y_send[:, cols] = value.astype(BF)
            else:
                total[:, cols] = value

        loop(tiles, body)

    sums(1)
    ry = remote(y_send, y_recv, ry_s, ry_r, y_peer)
    ry.start()
    for d in range(1, SIDE):
        ra_copy(d, 0).wait_recv()
    sums(0)
    ry.wait_recv()

    def finish(n):
        cols = tile(n)
        total[:, cols] = total[:, cols] + y_recv[:, cols].astype(F32)
        part[0, 0:rows, cols] = total[:, cols].astype(BF)

    loop(tiles, finish)
    last = pltpu.make_async_copy(part.at[0, 0:rows], mixed, mix_sem)
    last.start()

    for copy in y_copies + e_copies + [ry]:
        copy.wait_send()
    for d in range(1, SIDE):
        for dy in range(2):
            for copy in a_copies[d, dy]:
                copy.wait_send()
            ra_copy(d, dy).wait_send()
    for d in range(SIDE):
        for t in range(1, TARGETS):
            b_copy(d, t).wait_send()
            rb_copy(d, t).wait_send()
    last.wait()


def shards(tokens, routes, gate_weights, w_gate, w_up, w_down, saved_inputs, saved_cotangent):
    rows, width = tokens.shape
    hidden = w_gate.shape[2]
    back_rows = saved_inputs.shape[1]
    anywhere = pl.BlockSpec(memory_space=pl.ANY)
    whole = pl.BlockSpec(memory_space=pltpu.VMEM)
    dma = pltpu.SemaphoreType.DMA
    vm = pltpu.VMEM
    return pl.pallas_call(
        kernel,
        out_shape=(
            jax.ShapeDtypeStruct((rows, width), BF),
            jax.ShapeDtypeStruct((1, width // 2, hidden), F32),
            jax.ShapeDtypeStruct((1, width // 2, hidden), F32),
            jax.ShapeDtypeStruct((1, hidden // 2, width), F32),
        ),
        in_specs=[whole, whole] + [anywhere] * 6,
        out_specs=(anywhere,) * 4,
        scratch_shapes=[
            vm((width, hidden), BF), vm((width, hidden), BF), vm((hidden, width), BF),
            vm((SIDE, 2 * rows, width), BF),
            vm((SIDE, 2, 128, rows), BF), vm((2, 128, rows), F32),
            vm((CHUNK, 2 * rows), F32), vm((CHUNK, 2 * rows), BF), vm((2 * rows, CHUNK), BF),
            vm((SIDE, CHUNK, width), BF), vm((SIDE, CHUNK, width), BF), vm((SIDE, CHUNK, width), BF),
            vm((SIDE, 2 * rows, width), BF), vm((SIDE - 1, 2 * rows, width), BF),
            vm((rows, width), BF), vm((rows, width), BF), vm((rows, width), F32),
            vm((2, back_rows, width), BF), vm((2, back_rows, width), BF),
            vm((2, back_rows, hidden), BF), vm((2, back_rows, hidden), BF), vm((2, back_rows, hidden), BF),
            vm((CHUNK, hidden), BF),
            vm((2, 2, TILE, hidden), F32), vm((2, hidden // 2, 512), F32),
            dma((6,)), dma((2,)), dma((2,)), dma((3, 4)), dma((3, 4)),
            dma((SIDE, TARGETS)), dma((SIDE, TARGETS)), dma((SIDE, TARGETS)), dma((SIDE, TARGETS)),
            dma((3, 2)), dma((3, 2)), dma(()), dma(()), dma((2,)), dma((2,)), dma((3, 2)), dma(()),
        ],
        compiler_params=pltpu.CompilerParams(
            collective_id=0, has_side_effects=True, vmem_limit_bytes=62 * 1024 * 1024
        ),
        cost_estimate=pl.CostEstimate(flops=22 * 10**9, bytes_accessed=40 * 10**6, transcendentals=2 * 10**6),
    )(routes.T, gate_weights.T, tokens, w_gate, w_up, w_down, saved_inputs, saved_cotangent)


def solution(mesh):
    return jax.shard_map(
        shards,
        mesh=mesh,
        in_specs=(
            P(("edp", "ep"), None),
            P(("edp", "ep"), None),
            P(("edp", "ep"), None),
            P("ep", None, None),
            P("ep", None, None),
            P("ep", None, None),
            P("ep", "edp", None),
            P("ep", "edp", None),
        ),
        out_specs=(
            P(("edp", "ep"), None),
            P("ep", "edp", None),
            P("ep", "edp", None),
            P("ep", "edp", None),
        ),
        check_vma=False,
    )
```

```python
import jax
import jax.numpy as jnp
from jax import lax
from jax.experimental import pallas as pl
from jax.experimental.pallas import tpu as pltpu
from jax.sharding import PartitionSpec as P

CAP = 24
SIDE = 4
TARGETS = 8
PAIR = 2 * CAP
CHUNK = TARGETS * PAIR
TILE = 256
GROUPS = 2
COLS = 2
SEAT = {(0, 0): (0, 0), (1, 0): (0, 1), (3, 0): (1, 0), (2, 0): (1, 1),
        (0, 1): (2, 0), (3, 1): (2, 1), (1, 1): (3, 0), (2, 1): (3, 1)}
BF = jnp.bfloat16
F32 = jnp.float32


def dot(a, b, dims=((1,), (0,))):
    return lax.dot_general(a, b, (dims, ((), ())), preferred_element_type=F32)


def tile(n, size=TILE):
    return pl.ds(pl.multiple_of(n * size, size), size)


def loop(count, body):
    def step(n, carry):
        body(n)
        return carry

    lax.fori_loop(0, count, step, 0)


def kernel(
    routes, gates, tokens, w_gate, w_up, w_down, saved_x, saved_y,
    mixed, grad_gate, grad_up, grad_down,
    wg, wu, wd, blocks, aux, aux32, hot, hot_lhs, mix_lhs, packed, recv, back, part, gathered, passed,
    y_send, y_recv, total, result, xs, ys, hid, dgs, dus, hbuf, stage_a, stage_b,
    load_sem, y_s, y_r, a_s, a_r, b_s, b_r, rb_s, rb_r, rp_s, rp_r, ra_s, ra_r, ry_s, ry_r, e_s, e_r, out_sem, mix_sem,
):
    width = blocks.shape[-1]
    rows = blocks.shape[1] // 2
    hidden_width = wg.shape[1]
    half_width = width // 2
    half_hidden = hidden_width // 2
    tiles = width // TILE
    per_group = tiles // GROUPS

    me = lax.axis_index("ep")
    replica = lax.axis_index("edp")
    core = lax.rem(me, 2)
    x = lax.rem(me // 2, SIDE)
    z = lax.rem(me // (2 * SIDE), SIDE)
    y = me // (2 * SIDE * SIDE)
    a = z * (1 - core) + x * core
    b = x * (1 - core) + z * core

    def place(yy, aa, bb, cc):
        aa = lax.rem(aa, SIDE)
        bb = lax.rem(bb, SIDE)
        zz = aa * (1 - core) + bb * core
        xx = bb * (1 - core) + aa * core
        return ((yy * SIDE + zz) * SIDE + xx) * 2 + cc

    def at(index):
        return (replica, index)

    y_peer = at(place(1 - y, a, b, core))
    edp_peer = (1 - replica, me)
    ahead = at(place(y, a + 1, b, core))
    behind = at(place(y, a + SIDE - 1, b, core))

    def forward_to(t):
        f, g = t // 2, t % 2
        return place(y, a, b + f, core if g == 0 else 1 - core)

    def forwarder(t):
        f, g = t // 2, t % 2
        if g == 0:
            return place(y, a, b + SIDE - f, core)
        return place(y, a + SIDE - f, b, 1 - core)

    loads = [
        pltpu.make_async_copy(tokens, blocks.at[0, 0:rows], load_sem.at[0]),
        pltpu.make_async_copy(saved_x.at[0], xs.at[0], load_sem.at[1]),
        pltpu.make_async_copy(saved_y.at[0], ys.at[0], load_sem.at[2]),
        pltpu.make_async_copy(w_gate.at[0], wg, load_sem.at[3]),
        pltpu.make_async_copy(w_up.at[0], wu, load_sem.at[4]),
        pltpu.make_async_copy(w_down.at[0], wd, load_sem.at[5]),
    ]
    for copy in loads:
        copy.start()

    barrier = pltpu.get_barrier_semaphore()
    peers = [y_peer, edp_peer, ahead, behind]
    peers += [at(place(y, a, b + d, core)) for d in range(1, SIDE)]
    peers += [at(place(y, a, b + d, 1 - core)) for d in range(SIDE)]
    peers += [at(place(y, a + d, b, 1 - core)) for d in range(1, SIDE)]
    for peer in peers:
        pl.semaphore_signal(barrier, inc=1, device_id=peer, device_id_type=pl.DeviceIdType.MESH)

    experts = TARGETS * TARGETS
    names = lax.broadcasted_iota(jnp.int32, (experts, rows), 0)
    named = jnp.zeros((experts, rows), F32)
    weight = jnp.zeros((experts, rows), F32)
    for k in range(routes.shape[0]):
        match = names == routes[k : k + 1, :]
        named = named + jnp.where(match, 1.0, 0.0)
        weight = weight + jnp.where(match, gates[k : k + 1, :], 0.0)
    earlier = (
        lax.broadcasted_iota(jnp.int32, (rows, rows), 0)
        < lax.broadcasted_iota(jnp.int32, (rows, rows), 1)
    )
    earlier = jnp.where(earlier, 1.0, 0.0).astype(BF)
    count = dot(named.astype(BF), earlier)
    aux[0, 0, 0:experts, :] = jnp.where(named > 0.5, count, -1.0).astype(BF)
    aux[0, 0, experts : 2 * experts, :] = weight.astype(BF)
    hot[...] = jnp.zeros_like(hot)

    with jax.named_scope("barrier"):
        pl.semaphore_wait(barrier, len(peers))
        loads[0].wait()

    def remote(src, dst, send, receive, peer):
        return pltpu.make_async_remote_copy(
            src_ref=src, dst_ref=dst, send_sem=send, recv_sem=receive,
            device_id=peer, device_id_type=pl.DeviceIdType.MESH,
        )

    def half(dy):
        return pl.ds(rows * dy, rows)

    def columns(c):
        return pl.ds(c * (width // COLS), width // COLS)

    def token_copies(source, target, peer, send, receive, c):
        k, i = source
        m, j = target
        copies = [remote(blocks.at[k, half(i), columns(c)], blocks.at[m, half(j), columns(c)],
                         send.at[c], receive.at[c], peer)]
        if c == 0:
            copies.append(remote(aux.at[k, i], aux.at[m, j], send.at[COLS], receive.at[COLS], peer))
        return copies

    def y_copy(c):
        return token_copies(SEAT[0, 0], SEAT[0, 1], y_peer, y_s, y_r, c)

    def a_copy(slot, dy, c):
        source, peer = SEAT[0, dy], ahead if slot == 1 else behind
        if slot == 2 and dy == 0:
            source, peer = (SEAT[1, 0], ahead) if c == 0 else (SEAT[3, 0], behind)
        elif slot == 2:
            source, peer = SEAT[2, 0], y_peer
        return token_copies(source, SEAT[slot, dy], peer, a_s.at[2 * slot - 2 + dy],
                            a_r.at[2 * slot - 2 + dy], c)

    def begin(copies):
        for copy in copies:
            copy.start()

    def arrived(copies, name):
        with jax.named_scope(name):
            for copy in copies:
                copy.wait_recv()

    def a_start(slot, dy, c):
        begin(a_copy(slot, dy, c))

    def a_wait(slot, dy, c):
        arrived(a_copy(slot, dy, c), f"await{slot}{dy}{c}")

    e_copies = [
        remote(xs.at[0], xs.at[1], e_s.at[0], e_r.at[0], edp_peer),
        remote(ys.at[0], ys.at[1], e_s.at[1], e_r.at[1], edp_peer),
    ]

    def backward(r):
        def body(n):
            cols = tile(n)
            g = dot(xs[r], wg[:, cols])
            u = dot(xs[r], wu[:, cols])
            dh = dot(ys[r], wd[cols, :], ((1,), (1,)))
            s = jax.nn.sigmoid(g)
            act = g * s
            hid[r, :, cols] = (act * u).astype(BF)
            dgs[r, :, cols] = (dh * u * s * (1.0 + g * (1.0 - s))).astype(BF)
            dus[r, :, cols] = (dh * act).astype(BF)

        with jax.named_scope(f"bwd{r}"):
            loop(hidden_width // TILE, body)

    def fill_hot(d, weighted):
        slots = lax.broadcasted_iota(jnp.int32, (CAP, rows), 0).astype(F32)
        for dy in range(2):
            aux32[dy] = aux[d, dy].astype(F32)
        for t in range(TARGETS):
            e = forward_to(t)
            for dy in range(2):
                hit = aux32[dy, pl.ds(e, 1), :] == slots
                value = aux32[dy, pl.ds(e + experts, 1), :] if weighted else 1.0
                at_row = PAIR * t + CAP * dy
                hot[at_row : at_row + CAP, rows * dy : rows * dy + rows] = jnp.where(hit, value, 0.0)

    def b_copy(d, t):
        span = pl.ds(PAIR * t, PAIR)
        return remote(packed.at[d, span], recv.at[d, span], b_s.at[d, t], b_r.at[d, t], at(forward_to(t)))

    def group(q):
        return pl.ds(q * per_group * TILE, per_group * TILE)

    def rb_copy(d, t, q):
        span = pl.ds(PAIR * t, PAIR)
        return remote(recv.at[d, span, group(q)], back.at[d, span, group(q)], rb_s.at[q * SIDE + d, t],
                      rb_r.at[q * SIDE + d, t], at(forwarder(t)))

    def pack(d):
        with jax.named_scope(f"pack{d}"):
            fill_hot(d, False)
            hot_lhs[...] = hot[...].astype(BF)

            def body(n):
                cols = tile(n)
                rows_out = dot(hot_lhs[...], blocks[d, :, cols]).astype(BF)
                packed[d, :, cols] = rows_out
                recv[d, 0:PAIR, cols] = rows_out[0:PAIR]

            loop(tiles, body)
            for t in (4, 5, 2, 3, 6, 7, 1):
                b_copy(d, t).start()

    def up(d):
        with jax.named_scope(f"upwait{d}"):
            for t in range(1, TARGETS):
                b_copy(d, t).wait_recv()

        def body(n):
            cols = tile(n)
            g = dot(recv[d], wg[:, cols])
            u = dot(recv[d], wu[:, cols])
            hbuf[d, :, cols] = (g * jax.nn.sigmoid(g) * u).astype(BF)

        with jax.named_scope(f"up{d}"):
            loop(hidden_width // TILE, body)

    def down(d, q):
        def body(n):
            cols = tile(n + q * per_group)
            out = dot(hbuf[d], wd[:, cols]).astype(BF)
            recv[d, :, cols] = out
            back[d, 0:PAIR, cols] = out[0:PAIR]

        with jax.named_scope(f"down{d}{q}"):
            loop(per_group, body)
            for t in (4, 5, 2, 3, 6, 7, 1):
                rb_copy(d, t, q).start()

    def mix(d):
        with jax.named_scope(f"mix{d}"):
            fill_hot(d, True)
            mix_lhs[d] = hot[...].T.astype(BF)

    def ra_copy(k, q):
        i = 1 if k in (0, 2) else 0
        dy = k // 2
        side = 0 if k in (0, 3) else 1
        return remote(part.at[k, half(i), group(q)], gathered.at[2 * dy + side, :, group(q)],
                      ra_s.at[k, q], ra_r.at[2 * dy + side, q], behind if side == 0 else ahead)

    def ra_wait(k, q):
        ra_copy(k, q).wait_recv()

    def rp_copy(k, q):
        peer = y_peer if k == 3 else (behind if q == 0 else ahead)
        return remote(part.at[k, half(1), group(q)], passed.at[k // 2, :, group(q)],
                      rp_s.at[k // 2, q], rp_r.at[k // 2, q], peer)

    def ry_copy(q):
        return remote(y_send.at[:, group(q)], y_recv.at[:, group(q)], ry_s.at[q], ry_r.at[q], y_peer)

    def returned(k, q):
        with jax.named_scope(f"rbwait{k}{q}"):
            for t in range(1, TARGETS):
                rb_copy(k, t, q).wait_recv()

    def each_tile(q, body):
        loop(per_group, lambda n: body(tile(n + q * per_group)))

    def third(q):
        returned(3, q)

        def body(cols):
            part[3, :, cols] = dot(mix_lhs[3], back[3, :, cols]).astype(BF)

        with jax.named_scope(f"third{q}"):
            each_tile(q, body)
            rp_copy(3, q).start()
            ra_copy(3, q).start()

    def second(q):
        returned(2, q)

        def body(cols):
            value = dot(mix_lhs[2], back[2, :, cols])
            part[2, half(1), cols] = value[rows : 2 * rows].astype(BF)
            total[:, cols] = value[0:rows]

        with jax.named_scope(f"second{q}"):
            each_tile(q, body)
            ra_copy(2, q).start()

    def first(q):
        returned(1, q)
        arrived([rp_copy(3, q)], f"rpwait3{q}")

        def body(cols):
            value = dot(mix_lhs[1], back[1, :, cols])
            part[1, half(1), cols] = (value[rows : 2 * rows] + passed[1, :, cols].astype(F32)).astype(BF)
            if q == 0:
                part[1, half(0), cols] = value[0:rows].astype(BF)

        with jax.named_scope(f"first{q}"):
            each_tile(q, body)
            rp_copy(1, q).start()
            if q == 0:
                ra_copy(1, q).start()

    def first_late():
        q = 1
        arrived([rp_copy(1, q)], f"rpwait1{q}")

        def body(cols):
            value = dot(mix_lhs[1, half(0), :], back[1, :, cols])
            part[1, half(0), cols] = (value + passed[0, :, cols].astype(F32)).astype(BF)

        with jax.named_scope("firstlate"):
            each_tile(q, body)
            ra_copy(1, q).start()

    def zeroth(q):
        returned(0, q)
        if q == 0:
            arrived([rp_copy(1, q)], f"rpwait1{q}")

        def body(cols):
            value = dot(mix_lhs[0], back[0, :, cols])
            rest = value[rows : 2 * rows]
            if q == 0:
                rest = rest + passed[0, :, cols].astype(F32)
            part[0, half(1), cols] = rest.astype(BF)
            total[:, cols] = value[0:rows]

        with jax.named_scope(f"zeroth{q}"):
            each_tile(q, body)
            ra_copy(0, q).start()

    def home(q):
        arrived([ra_copy(3, q), ra_copy(2, q)], f"rawait{q}")

        def body(cols):
            value = total[:, cols] + gathered[2, :, cols].astype(F32) + gathered[3, :, cols].astype(F32)
            y_send[:, cols] = value.astype(BF)

        with jax.named_scope(f"home{q}"):
            each_tile(q, body)
            ry_copy(q).start()

    def mixed_copy(q):
        return pltpu.make_async_copy(result.at[:, group(q)], mixed.at[:, group(q)], mix_sem.at[q])

    def finish(q):
        arrived([ry_copy(q), ra_copy(1, q), ra_copy(0, q)], f"lastwait{q}")

        def body(cols):
            value = total[:, cols] + y_recv[:, cols].astype(F32)
            value = value + gathered[0, :, cols].astype(F32) + gathered[1, :, cols].astype(F32)
            result[:, cols] = value.astype(BF)

        each_tile(q, body)
        mixed_copy(q).start()

    def out_copies(kind, n):
        slot = lax.rem(n, 2)
        if kind == 2:
            return pltpu.make_async_copy(stage_b.at[slot], grad_down.at[0, :, tile(n, stage_b.shape[2])],
                                         out_sem.at[2, slot])
        ref = grad_gate if kind == 0 else grad_up
        return pltpu.make_async_copy(stage_a.at[kind, slot], ref.at[0, tile(n)], out_sem.at[kind, slot])

    def in_weight_grads():
        def body(n):
            @pl.when(n >= 2)
            def _():
                for kind in range(2):
                    out_copies(kind, n - 2).wait()

            cols = pl.ds(pl.multiple_of(replica * half_width + n * TILE, TILE), TILE)
            slot = lax.rem(n, 2)
            for kind, source in ((0, dgs), (1, dus)):
                sums = [dot(xs[r, :, cols], source[r], ((0,), (0,))).astype(BF).astype(F32) for r in range(2)]
                stage_a[kind, slot] = sums[0] + sums[1]
                out_copies(kind, n).start()

        count = half_width // TILE
        with jax.named_scope("gradin"):
            loop(count, body)
            for n in (count - 2, count - 1):
                for kind in range(2):
                    out_copies(kind, n).wait()

    def down_weight_grad():
        size = stage_b.shape[2]

        def body(n):
            @pl.when(n >= 2)
            def _():
                out_copies(2, n - 2).wait()

            own_cols = pl.ds(pl.multiple_of(replica * half_hidden, 128), half_hidden)
            slot = lax.rem(n, 2)
            sums = [
                dot(hid[r, :, own_cols], ys[r, :, tile(n, size)], ((0,), (0,))).astype(BF).astype(F32)
                for r in range(2)
            ]
            stage_b[slot] = sums[0] + sums[1]
            out_copies(2, n).start()

        with jax.named_scope("graddown"):
            loop(width // size, body)
            for n in (width // size - 2, width // size - 1):
                out_copies(2, n).wait()

    begin(y_copy(0))
    a_start(1, 0, 0)
    a_start(3, 0, 1)
    a_start(1, 0, 1)
    a_start(3, 0, 0)
    begin(y_copy(1))
    with jax.named_scope("wload"):
        for copy in loads[1:]:
            copy.wait()
    backward(0)
    a_wait(1, 0, 0)
    a_start(2, 0, 0)
    a_wait(3, 0, 1)
    a_start(2, 0, 1)
    arrived(y_copy(0), "ywait0")
    a_start(1, 1, 0)
    a_start(3, 1, 0)
    a_wait(1, 0, 1)
    pack(0)
    for c in range(COLS):
        a_wait(2, 0, c)
        a_start(2, 1, c)
    begin(e_copies)
    arrived(y_copy(1), "ywait1")
    a_start(1, 1, 1)
    a_start(3, 1, 1)
    a_wait(3, 0, 0)
    pack(1)
    for c in range(COLS):
        a_wait(3, 1, c)
    pack(2)
    for c in range(COLS):
        a_wait(1, 1, c)
        a_wait(2, 1, c)
    pack(3)
    up(0)
    mix(3)
    mix(2)
    up(1)
    mix(1)
    mix(0)
    up(2)
    for q in range(GROUPS):
        down(2, q)
    up(3)
    for k in (3, 1, 0):
        for q in range(GROUPS):
            down(k, q)
    for q in range(GROUPS):
        third(q)
    for q in range(GROUPS):
        second(q)
    arrived(e_copies, "ewait")
    backward(1)
    for q in (1, 0):
        first(q)
    in_weight_grads()
    down_weight_grad()
    for q in range(GROUPS):
        home(q)
    zeroth(1)
    first_late()
    zeroth(0)
    finish(1)
    finish(0)

    for copy in e_copies:
        copy.wait_send()
    for c in range(COLS):
        for copy in y_copy(c):
            copy.wait_send()
        for slot in range(1, SIDE):
            for dy in range(2):
                for copy in a_copy(slot, dy, c):
                    copy.wait_send()
    for d in range(SIDE):
        for t in range(1, TARGETS):
            b_copy(d, t).wait_send()
    for q in range(GROUPS):
        for k in range(SIDE):
            for t in range(1, TARGETS):
                rb_copy(k, t, q).wait_send()
            ra_copy(k, q).wait_send()
        for k in (1, 3):
            rp_copy(k, q).wait_send()
        ry_copy(q).wait_send()
        mixed_copy(q).wait()


def shards(tokens, routes, gate_weights, w_gate, w_up, w_down, saved_inputs, saved_cotangent):
    rows, width = tokens.shape
    hidden = w_gate.shape[2]
    back_rows = saved_inputs.shape[1]
    anywhere = pl.BlockSpec(memory_space=pl.ANY)
    whole = pl.BlockSpec(memory_space=pltpu.VMEM)
    dma = pltpu.SemaphoreType.DMA
    vm = pltpu.VMEM
    return pl.pallas_call(
        kernel,
        out_shape=(
            jax.ShapeDtypeStruct((rows, width), BF),
            jax.ShapeDtypeStruct((1, width // 2, hidden), F32),
            jax.ShapeDtypeStruct((1, width // 2, hidden), F32),
            jax.ShapeDtypeStruct((1, hidden // 2, width), F32),
        ),
        in_specs=[whole, whole] + [anywhere] * 6,
        out_specs=(anywhere,) * 4,
        scratch_shapes=[
            vm((width, hidden), BF), vm((width, hidden), BF), vm((hidden, width), BF),
            vm((SIDE, 2 * rows, width), BF),
            vm((SIDE, 2, 128, rows), BF), vm((2, 128, rows), F32),
            vm((CHUNK, 2 * rows), F32), vm((CHUNK, 2 * rows), BF), vm((SIDE, 2 * rows, CHUNK), BF),
            vm((SIDE, CHUNK, width), BF), vm((SIDE, CHUNK, width), BF), vm((SIDE, CHUNK, width), BF),
            vm((SIDE, 2 * rows, width), BF), vm((SIDE, rows, width), BF), vm((2, rows, width), BF),
            vm((rows, width), BF), vm((rows, width), BF), vm((rows, width), F32), vm((rows, width), BF),
            vm((2, back_rows, width), BF), vm((2, back_rows, width), BF),
            vm((2, back_rows, hidden), BF), vm((2, back_rows, hidden), BF), vm((2, back_rows, hidden), BF),
            vm((SIDE, CHUNK, hidden), BF),
            vm((2, 2, TILE, hidden), F32), vm((2, hidden // 2, 512), F32),
            dma((6,)), dma((COLS + 1,)), dma((COLS + 1,)), dma((6, COLS + 1)), dma((6, COLS + 1)),
            dma((SIDE, TARGETS)), dma((SIDE, TARGETS)),
            dma((SIDE * GROUPS, TARGETS)), dma((SIDE * GROUPS, TARGETS)),
            dma((2, GROUPS)), dma((2, GROUPS)), dma((SIDE, GROUPS)), dma((SIDE, GROUPS)),
            dma((GROUPS,)), dma((GROUPS,)), dma((2,)), dma((2,)), dma((3, 2)), dma((GROUPS,)),
        ],
        compiler_params=pltpu.CompilerParams(
            collective_id=0, has_side_effects=True, vmem_limit_bytes=62 * 1024 * 1024
        ),
        cost_estimate=pl.CostEstimate(flops=22 * 10**9, bytes_accessed=40 * 10**6, transcendentals=2 * 10**6),
    )(routes.T, gate_weights.T, tokens, w_gate, w_up, w_down, saved_inputs, saved_cotangent)


def solution(mesh):
    return jax.shard_map(
        shards,
        mesh=mesh,
        in_specs=(
            P(("edp", "ep"), None),
            P(("edp", "ep"), None),
            P(("edp", "ep"), None),
            P("ep", None, None),
            P("ep", None, None),
            P("ep", None, None),
            P("ep", "edp", None),
            P("ep", "edp", None),
        ),
        out_specs=(
            P(("edp", "ep"), None),
            P("ep", "edp", None),
            P("ep", "edp", None),
            P("ep", "edp", None),
        ),
        check_vma=False,
    )
```

```python
import jax
import jax.numpy as jnp
from jax import lax
from jax.experimental import pallas as pl
from jax.experimental.pallas import tpu as pltpu
from jax.sharding import PartitionSpec as P

CAP = 24
SIDE = 4
TARGETS = 8
PAIR = 2 * CAP
CHUNK = TARGETS * PAIR
TILE = 256
GROUPS = 2
COLS = 2
SEAT = {(0, 0): (0, 0), (1, 0): (0, 1), (3, 0): (1, 0), (2, 0): (1, 1),
        (0, 1): (2, 0), (3, 1): (2, 1), (1, 1): (3, 0), (2, 1): (3, 1)}
BF = jnp.bfloat16
F32 = jnp.float32


def dot(a, b, dims=((1,), (0,))):
    return lax.dot_general(a, b, (dims, ((), ())), preferred_element_type=F32)


def tile(n, size=TILE):
    return pl.ds(pl.multiple_of(n * size, size), size)


def loop(count, body):
    def step(n, carry):
        body(n)
        return carry

    lax.fori_loop(0, count, step, 0)


def kernel(
    routes, gates, tokens, w_gate, w_up, w_down, saved_x, saved_y,
    mixed, grad_gate, grad_up, grad_down,
    wg, wu, wd, blocks, aux, aux32, hot, hot_lhs, mix_lhs, packed, recv, back, part, gathered, passed,
    y_send, y_recv, total, xs, ys, hid, dgs, dus, hbuf,
    load_sem, y_s, y_r, a_s, a_r, b_s, b_r, rb_s, rb_r, rp_s, rp_r, ra_s, ra_r, ry_s, ry_r, e_s, e_r,
):
    width = blocks.shape[-1]
    rows = blocks.shape[1] // 2
    hidden_width = wg.shape[1]
    half_width = width // 2
    half_hidden = hidden_width // 2
    tiles = width // TILE
    per_group = tiles // GROUPS

    me = lax.axis_index("ep")
    replica = lax.axis_index("edp")
    core = lax.rem(me, 2)
    x = lax.rem(me // 2, SIDE)
    z = lax.rem(me // (2 * SIDE), SIDE)
    y = me // (2 * SIDE * SIDE)
    a = z * (1 - core) + x * core
    b = x * (1 - core) + z * core

    def place(yy, aa, bb, cc):
        aa = lax.rem(aa, SIDE)
        bb = lax.rem(bb, SIDE)
        zz = aa * (1 - core) + bb * core
        xx = bb * (1 - core) + aa * core
        return ((yy * SIDE + zz) * SIDE + xx) * 2 + cc

    def at(index):
        return (replica, index)

    y_peer = at(place(1 - y, a, b, core))
    edp_peer = (1 - replica, me)
    ahead = at(place(y, a + 1, b, core))
    behind = at(place(y, a + SIDE - 1, b, core))

    def forward_to(t):
        f, g = t // 2, t % 2
        return place(y, a, b + f, core if g == 0 else 1 - core)

    def forwarder(t):
        f, g = t // 2, t % 2
        if g == 0:
            return place(y, a, b + SIDE - f, core)
        return place(y, a + SIDE - f, b, 1 - core)

    loads = [
        pltpu.make_async_copy(tokens, blocks.at[0, 0:rows], load_sem.at[0]),
        pltpu.make_async_copy(saved_x.at[0], xs.at[0], load_sem.at[1]),
        pltpu.make_async_copy(saved_y.at[0], ys.at[0], load_sem.at[2]),
        pltpu.make_async_copy(w_gate.at[0], wg, load_sem.at[3]),
        pltpu.make_async_copy(w_up.at[0], wu, load_sem.at[4]),
        pltpu.make_async_copy(w_down.at[0], wd, load_sem.at[5]),
    ]
    for copy in loads:
        copy.start()

    barrier = pltpu.get_barrier_semaphore()
    peers = [y_peer, edp_peer, ahead, behind]
    peers += [at(place(y, a, b + d, core)) for d in range(1, SIDE)]
    peers += [at(place(y, a, b + d, 1 - core)) for d in range(SIDE)]
    peers += [at(place(y, a + d, b, 1 - core)) for d in range(1, SIDE)]
    for peer in peers:
        pl.semaphore_signal(barrier, inc=1, device_id=peer, device_id_type=pl.DeviceIdType.MESH)

    experts = TARGETS * TARGETS
    names = lax.broadcasted_iota(jnp.int32, (experts, rows), 0)
    named = jnp.zeros((experts, rows), F32)
    weight = jnp.zeros((experts, rows), F32)
    for k in range(routes.shape[0]):
        match = names == routes[k : k + 1, :]
        named = named + jnp.where(match, 1.0, 0.0)
        weight = weight + jnp.where(match, gates[k : k + 1, :], 0.0)
    earlier = (
        lax.broadcasted_iota(jnp.int32, (rows, rows), 0)
        < lax.broadcasted_iota(jnp.int32, (rows, rows), 1)
    )
    earlier = jnp.where(earlier, 1.0, 0.0).astype(BF)
    count = dot(named.astype(BF), earlier)
    aux[0, 0, 0:experts, :] = jnp.where(named > 0.5, count, -1.0).astype(BF)
    aux[0, 0, experts : 2 * experts, :] = weight.astype(BF)
    hot[...] = jnp.zeros_like(hot)

    with jax.named_scope("barrier"):
        pl.semaphore_wait(barrier, len(peers))
        loads[0].wait()

    def remote(src, dst, send, receive, peer):
        return pltpu.make_async_remote_copy(
            src_ref=src, dst_ref=dst, send_sem=send, recv_sem=receive,
            device_id=peer, device_id_type=pl.DeviceIdType.MESH,
        )

    def half(dy):
        return pl.ds(rows * dy, rows)

    def columns(c):
        return pl.ds(c * (width // COLS), width // COLS)

    def token_copies(source, target, peer, send, receive, c):
        k, i = source
        m, j = target
        copies = [remote(blocks.at[k, half(i), columns(c)], blocks.at[m, half(j), columns(c)],
                         send.at[c], receive.at[c], peer)]
        if c == 0:
            copies.append(remote(aux.at[k, i], aux.at[m, j], send.at[COLS], receive.at[COLS], peer))
        return copies

    def y_copy(c):
        return token_copies(SEAT[0, 0], SEAT[0, 1], y_peer, y_s, y_r, c)

    def a_copy(slot, dy, c):
        source, peer = SEAT[0, dy], ahead if slot == 1 else behind
        if slot == 2 and dy == 0:
            source, peer = (SEAT[1, 0], ahead) if c == 0 else (SEAT[3, 0], behind)
        elif slot == 2:
            source, peer = SEAT[2, 0], y_peer
        return token_copies(source, SEAT[slot, dy], peer, a_s.at[2 * slot - 2 + dy],
                            a_r.at[2 * slot - 2 + dy], c)

    def begin(copies):
        for copy in copies:
            copy.start()

    def arrived(copies, name):
        with jax.named_scope(name):
            for copy in copies:
                copy.wait_recv()

    def a_start(slot, dy, c):
        begin(a_copy(slot, dy, c))

    def a_wait(slot, dy, c):
        arrived(a_copy(slot, dy, c), f"await{slot}{dy}{c}")

    e_copies = [
        remote(xs.at[0], xs.at[1], e_s.at[0], e_r.at[0], edp_peer),
        remote(ys.at[0], ys.at[1], e_s.at[1], e_r.at[1], edp_peer),
    ]

    def backward(r):
        def body(n):
            cols = tile(n)
            g = dot(xs[r], wg[:, cols])
            u = dot(xs[r], wu[:, cols])
            dh = dot(ys[r], wd[cols, :], ((1,), (1,)))
            s = jax.nn.sigmoid(g)
            act = g * s
            hid[r, :, cols] = (act * u).astype(BF)
            dgs[r, :, cols] = (dh * u * s * (1.0 + g * (1.0 - s))).astype(BF)
            dus[r, :, cols] = (dh * act).astype(BF)

        with jax.named_scope(f"bwd{r}"):
            loop(hidden_width // TILE, body)

    def fill_hot(d, weighted):
        slots = lax.broadcasted_iota(jnp.int32, (CAP, rows), 0).astype(F32)
        for dy in range(2):
            aux32[dy] = aux[d, dy].astype(F32)
        for t in range(TARGETS):
            e = forward_to(t)
            for dy in range(2):
                hit = aux32[dy, pl.ds(e, 1), :] == slots
                value = aux32[dy, pl.ds(e + experts, 1), :] if weighted else 1.0
                at_row = PAIR * t + CAP * dy
                hot[at_row : at_row + CAP, rows * dy : rows * dy + rows] = jnp.where(hit, value, 0.0)

    def b_copy(d, t):
        span = pl.ds(PAIR * t, PAIR)
        return remote(packed.at[d, span], recv.at[d, span], b_s.at[d, t], b_r.at[d, t], at(forward_to(t)))

    def group(q):
        return pl.ds(q * per_group * TILE, per_group * TILE)

    def rb_copy(d, t, q):
        span = pl.ds(PAIR * t, PAIR)
        return remote(recv.at[d, span, group(q)], back.at[d, span, group(q)], rb_s.at[q * SIDE + d, t],
                      rb_r.at[q * SIDE + d, t], at(forwarder(t)))

    def pack(d):
        with jax.named_scope(f"pack{d}"):
            fill_hot(d, False)
            hot_lhs[...] = hot[...].astype(BF)

            def body(n):
                cols = tile(n)
                rows_out = dot(hot_lhs[...], blocks[d, :, cols]).astype(BF)
                packed[d, :, cols] = rows_out
                recv[d, 0:PAIR, cols] = rows_out[0:PAIR]

            loop(tiles, body)
            for t in (4, 5, 2, 3, 6, 7, 1):
                b_copy(d, t).start()

    def up(d):
        with jax.named_scope(f"upwait{d}"):
            for t in range(1, TARGETS):
                b_copy(d, t).wait_recv()

        def body(n):
            cols = tile(n)
            g = dot(recv[d], wg[:, cols])
            u = dot(recv[d], wu[:, cols])
            hbuf[d, :, cols] = (g * jax.nn.sigmoid(g) * u).astype(BF)

        with jax.named_scope(f"up{d}"):
            loop(hidden_width // TILE, body)

    def down(d, q):
        def body(n):
            cols = tile(n + q * per_group)
            out = dot(hbuf[d], wd[:, cols]).astype(BF)
            recv[d, :, cols] = out
            back[d, 0:PAIR, cols] = out[0:PAIR]

        with jax.named_scope(f"down{d}{q}"):
            loop(per_group, body)
            for t in (4, 5, 2, 3, 6, 7, 1):
                rb_copy(d, t, q).start()

    def mix(d):
        with jax.named_scope(f"mix{d}"):
            fill_hot(d, True)
            mix_lhs[d] = hot[...].T.astype(BF)

    def ra_copy(k, q):
        i = 1 if k in (0, 2) else 0
        dy = k // 2
        side = 0 if k in (0, 3) else 1
        return remote(part.at[k, half(i), group(q)], gathered.at[2 * dy + side, :, group(q)],
                      ra_s.at[k, q], ra_r.at[2 * dy + side, q], behind if side == 0 else ahead)

    def ra_wait(k, q):
        ra_copy(k, q).wait_recv()

    def rp_copy(k, q):
        peer = y_peer if k == 3 else (behind if q == 0 else ahead)
        return remote(part.at[k, half(1), group(q)], passed.at[k // 2, :, group(q)],
                      rp_s.at[k // 2, q], rp_r.at[k // 2, q], peer)

    def ry_copy(q):
        return remote(y_send.at[:, group(q)], y_recv.at[:, group(q)], ry_s.at[q], ry_r.at[q], y_peer)

    def returned(k, q):
        with jax.named_scope(f"rbwait{k}{q}"):
            for t in range(1, TARGETS):
                rb_copy(k, t, q).wait_recv()

    def each_tile(q, body):
        loop(per_group, lambda n: body(tile(n + q * per_group)))

    def third(q):
        returned(3, q)

        def body(cols):
            part[3, :, cols] = dot(mix_lhs[3], back[3, :, cols]).astype(BF)

        with jax.named_scope(f"third{q}"):
            each_tile(q, body)
            rp_copy(3, q).start()
            ra_copy(3, q).start()

    def second(q):
        returned(2, q)

        def body(cols):
            value = dot(mix_lhs[2], back[2, :, cols])
            part[2, half(1), cols] = value[rows : 2 * rows].astype(BF)
            total[:, cols] = value[0:rows]

        with jax.named_scope(f"second{q}"):
            each_tile(q, body)
            ra_copy(2, q).start()

    def first(q):
        returned(1, q)
        arrived([rp_copy(3, q)], f"rpwait3{q}")

        def body(cols):
            value = dot(mix_lhs[1], back[1, :, cols])
            part[1, half(1), cols] = (value[rows : 2 * rows] + passed[1, :, cols].astype(F32)).astype(BF)
            if q == 0:
                part[1, half(0), cols] = value[0:rows].astype(BF)

        with jax.named_scope(f"first{q}"):
            each_tile(q, body)
            rp_copy(1, q).start()
            if q == 0:
                ra_copy(1, q).start()

    def first_late():
        q = 1
        arrived([rp_copy(1, q)], f"rpwait1{q}")

        def body(cols):
            value = dot(mix_lhs[1, half(0), :], back[1, :, cols])
            part[1, half(0), cols] = (value + passed[0, :, cols].astype(F32)).astype(BF)

        with jax.named_scope("firstlate"):
            each_tile(q, body)
            ra_copy(1, q).start()

    def zeroth(q):
        returned(0, q)
        if q == 0:
            arrived([rp_copy(1, q)], f"rpwait1{q}")

        def body(cols):
            value = dot(mix_lhs[0], back[0, :, cols])
            rest = value[rows : 2 * rows]
            if q == 0:
                rest = rest + passed[0, :, cols].astype(F32)
            part[0, half(1), cols] = rest.astype(BF)
            total[:, cols] = value[0:rows]

        with jax.named_scope(f"zeroth{q}"):
            each_tile(q, body)
            ra_copy(0, q).start()

    def home(q):
        arrived([ra_copy(3, q), ra_copy(2, q)], f"rawait{q}")

        def body(cols):
            value = total[:, cols] + gathered[2, :, cols].astype(F32) + gathered[3, :, cols].astype(F32)
            y_send[:, cols] = value.astype(BF)

        with jax.named_scope(f"home{q}"):
            each_tile(q, body)
            ry_copy(q).start()

    def finish(q):
        arrived([ry_copy(q), ra_copy(1, q), ra_copy(0, q)], f"lastwait{q}")

        def body(cols):
            value = total[:, cols] + y_recv[:, cols].astype(F32)
            value = value + gathered[0, :, cols].astype(F32) + gathered[1, :, cols].astype(F32)
            mixed[:, cols] = value.astype(BF)

        each_tile(q, body)

    def in_weight_grads():
        def body(n):
            cols = pl.ds(pl.multiple_of(replica * half_width + n * TILE, TILE), TILE)
            for out, source in ((grad_gate, dgs), (grad_up, dus)):
                sums = [dot(xs[r, :, cols], source[r], ((0,), (0,))).astype(BF).astype(F32) for r in range(2)]
                out[0, tile(n), :] = sums[0] + sums[1]

        with jax.named_scope("gradin"):
            loop(half_width // TILE, body)

    def down_weight_grad():
        size = 512

        def body(n):
            own_cols = pl.ds(pl.multiple_of(replica * half_hidden, 128), half_hidden)
            sums = [
                dot(hid[r, :, own_cols], ys[r, :, tile(n, size)], ((0,), (0,))).astype(BF).astype(F32)
                for r in range(2)
            ]
            grad_down[0, :, tile(n, size)] = sums[0] + sums[1]

        with jax.named_scope("graddown"):
            loop(width // size, body)

    begin(y_copy(0))
    a_start(1, 0, 0)
    a_start(3, 0, 1)
    a_start(1, 0, 1)
    a_start(3, 0, 0)
    begin(y_copy(1))
    with jax.named_scope("wload"):
        for copy in loads[1:]:
            copy.wait()
    backward(0)
    a_wait(1, 0, 0)
    a_start(2, 0, 0)
    a_wait(3, 0, 1)
    a_start(2, 0, 1)
    arrived(y_copy(0), "ywait0")
    a_start(1, 1, 0)
    a_start(3, 1, 0)
    a_wait(1, 0, 1)
    pack(0)
    for c in range(COLS):
        a_wait(2, 0, c)
        a_start(2, 1, c)
    begin(e_copies)
    arrived(y_copy(1), "ywait1")
    a_start(1, 1, 1)
    a_start(3, 1, 1)
    a_wait(3, 0, 0)
    pack(1)
    for c in range(COLS):
        a_wait(3, 1, c)
    pack(2)
    for c in range(COLS):
        a_wait(1, 1, c)
        a_wait(2, 1, c)
    pack(3)
    up(0)
    mix(3)
    mix(2)
    up(1)
    mix(1)
    mix(0)
    up(2)
    for q in range(GROUPS):
        down(2, q)
    up(3)
    for k in (3, 1, 0):
        for q in range(GROUPS):
            down(k, q)
    for q in range(GROUPS):
        third(q)
    for q in range(GROUPS):
        second(q)
    arrived(e_copies, "ewait")
    backward(1)
    for q in (1, 0):
        first(q)
    in_weight_grads()
    down_weight_grad()
    for q in range(GROUPS):
        home(q)
    zeroth(1)
    first_late()
    zeroth(0)
    finish(1)
    finish(0)

    for copy in e_copies:
        copy.wait_send()
    for c in range(COLS):
        for copy in y_copy(c):
            copy.wait_send()
        for slot in range(1, SIDE):
            for dy in range(2):
                for copy in a_copy(slot, dy, c):
                    copy.wait_send()
    for d in range(SIDE):
        for t in range(1, TARGETS):
            b_copy(d, t).wait_send()
    for q in range(GROUPS):
        for k in range(SIDE):
            for t in range(1, TARGETS):
                rb_copy(k, t, q).wait_send()
            ra_copy(k, q).wait_send()
        for k in (1, 3):
            rp_copy(k, q).wait_send()
        ry_copy(q).wait_send()


def flush(*refs):
    count = len(refs) // 2
    sems = refs[-1]
    copies = [
        pltpu.make_async_copy(source, target, sems.at[n])
        for n, (source, target) in enumerate(zip(refs[:count], refs[count : 2 * count]))
    ]
    for copy in copies:
        copy.start()
    for copy in copies:
        copy.wait()


def shards(tokens, routes, gate_weights, w_gate, w_up, w_down, saved_inputs, saved_cotangent):
    rows, width = tokens.shape
    hidden = w_gate.shape[2]
    back_rows = saved_inputs.shape[1]
    anywhere = pl.BlockSpec(memory_space=pl.ANY)
    whole = pl.BlockSpec(memory_space=pltpu.VMEM)
    dma = pltpu.SemaphoreType.DMA
    vm = pltpu.VMEM
    held = pl.pallas_call(
        kernel,
        out_shape=(
            pltpu.VMEM((rows, width), BF),
            pltpu.VMEM((1, width // 2, hidden), F32),
            pltpu.VMEM((1, width // 2, hidden), F32),
            pltpu.VMEM((1, hidden // 2, width), F32),
        ),
        in_specs=[whole, whole] + [anywhere] * 6,
        out_specs=(whole,) * 4,
        scratch_shapes=[
            vm((width, hidden), BF), vm((width, hidden), BF), vm((hidden, width), BF),
            vm((SIDE, 2 * rows, width), BF),
            vm((SIDE, 2, 128, rows), BF), vm((2, 128, rows), F32),
            vm((CHUNK, 2 * rows), F32), vm((CHUNK, 2 * rows), BF), vm((SIDE, 2 * rows, CHUNK), BF),
            vm((SIDE, CHUNK, width), BF), vm((SIDE, CHUNK, width), BF), vm((SIDE, CHUNK, width), BF),
            vm((SIDE, 2 * rows, width), BF), vm((SIDE, rows, width), BF), vm((2, rows, width), BF),
            vm((rows, width), BF), vm((rows, width), BF), vm((rows, width), F32),
            vm((2, back_rows, width), BF), vm((2, back_rows, width), BF),
            vm((2, back_rows, hidden), BF), vm((2, back_rows, hidden), BF), vm((2, back_rows, hidden), BF),
            vm((SIDE, CHUNK, hidden), BF),
            dma((6,)), dma((COLS + 1,)), dma((COLS + 1,)), dma((6, COLS + 1)), dma((6, COLS + 1)),
            dma((SIDE, TARGETS)), dma((SIDE, TARGETS)),
            dma((SIDE * GROUPS, TARGETS)), dma((SIDE * GROUPS, TARGETS)),
            dma((2, GROUPS)), dma((2, GROUPS)), dma((SIDE, GROUPS)), dma((SIDE, GROUPS)),
            dma((GROUPS,)), dma((GROUPS,)), dma((2,)), dma((2,)),
        ],
        compiler_params=pltpu.CompilerParams(
            collective_id=0, has_side_effects=True, vmem_limit_bytes=53 * 1024 * 1024
        ),
        cost_estimate=pl.CostEstimate(flops=22 * 10**9, bytes_accessed=40 * 10**6, transcendentals=2 * 10**6),
    )(routes.T, gate_weights.T, tokens, w_gate, w_up, w_down, saved_inputs, saved_cotangent)
    return pl.pallas_call(
        flush,
        out_shape=tuple(jax.ShapeDtypeStruct(h.shape, h.dtype) for h in held),
        in_specs=[anywhere] * 4,
        out_specs=(anywhere,) * 4,
        scratch_shapes=[dma((4,))],
        compiler_params=pltpu.CompilerParams(vmem_limit_bytes=1024 * 1024),
        cost_estimate=pl.CostEstimate(flops=0, bytes_accessed=20 * 10**6, transcendentals=0),
    )(*[pltpu.with_memory_space_constraint(h, pltpu.VMEM) for h in held])


def solution(mesh):
    return jax.shard_map(
        shards,
        mesh=mesh,
        in_specs=(
            P(("edp", "ep"), None),
            P(("edp", "ep"), None),
            P(("edp", "ep"), None),
            P("ep", None, None),
            P("ep", None, None),
            P("ep", None, None),
            P("ep", "edp", None),
            P("ep", "edp", None),
        ),
        out_specs=(
            P(("edp", "ep"), None),
            P("ep", "edp", None),
            P("ep", "edp", None),
            P("ep", "edp", None),
        ),
        check_vma=False,
    )
```

```python
import jax
import jax.numpy as jnp
from jax import lax
from jax.experimental import pallas as pl
from jax.experimental.pallas import tpu as pltpu
from jax.sharding import PartitionSpec as P

CAP = 24
SIDE = 4
TARGETS = 8
PAIR = 2 * CAP
CHUNK = TARGETS * PAIR
TILE = 256
GROUPS = 2
COLS = 2
SEAT = {(0, 0): (0, 0), (1, 0): (0, 1), (3, 0): (1, 0), (2, 0): (1, 1),
        (0, 1): (2, 0), (3, 1): (2, 1), (1, 1): (3, 0), (2, 1): (3, 1)}
BF = jnp.bfloat16
F32 = jnp.float32


def dot(a, b, dims=((1,), (0,))):
    return lax.dot_general(a, b, (dims, ((), ())), preferred_element_type=F32)


def tile(n, size=TILE):
    return pl.ds(pl.multiple_of(n * size, size), size)


def loop(count, body):
    def step(n, carry):
        body(n)
        return carry

    lax.fori_loop(0, count, step, 0)


def kernel(
    routes, gates, tokens, w_gate, w_up, w_down, saved_x, saved_y,
    mixed, grad_gate, grad_up, grad_down,
    wg, wu, wd, blocks, aux, aux32, hot, hot_lhs, mix_lhs, packed, recv, back, part, gathered, passed,
    y_send, y_recv, total, xs, ys, hid, dgs, dus, hbuf,
    load_sem, y_s, y_r, a_s, a_r, b_s, b_r, rb_s, rb_r, rp_s, rp_r, ra_s, ra_r, ry_s, ry_r, e_s, e_r,
):
    width = blocks.shape[-1]
    rows = blocks.shape[1] // 2
    hidden_width = wg.shape[1]
    half_width = width // 2
    half_hidden = hidden_width // 2
    tiles = width // TILE
    per_group = tiles // GROUPS

    me = lax.axis_index("ep")
    replica = lax.axis_index("edp")
    core = lax.rem(me, 2)
    x = lax.rem(me // 2, SIDE)
    z = lax.rem(me // (2 * SIDE), SIDE)
    y = me // (2 * SIDE * SIDE)
    a = z * (1 - core) + x * core
    b = x * (1 - core) + z * core

    def place(yy, aa, bb, cc):
        aa = lax.rem(aa, SIDE)
        bb = lax.rem(bb, SIDE)
        zz = aa * (1 - core) + bb * core
        xx = bb * (1 - core) + aa * core
        return ((yy * SIDE + zz) * SIDE + xx) * 2 + cc

    def at(index):
        return (replica, index)

    y_peer = at(place(1 - y, a, b, core))
    edp_peer = (1 - replica, me)
    ahead = at(place(y, a + 1, b, core))
    behind = at(place(y, a + SIDE - 1, b, core))

    def forward_to(t):
        f, g = t // 2, t % 2
        return place(y, a, b + f, core if g == 0 else 1 - core)

    def forwarder(t):
        f, g = t // 2, t % 2
        if g == 0:
            return place(y, a, b + SIDE - f, core)
        return place(y, a + SIDE - f, b, 1 - core)

    loads = [
        pltpu.make_async_copy(tokens, blocks.at[0, 0:rows], load_sem.at[0]),
        pltpu.make_async_copy(saved_x.at[0], xs.at[0], load_sem.at[1]),
        pltpu.make_async_copy(saved_y.at[0], ys.at[0], load_sem.at[2]),
        pltpu.make_async_copy(w_gate.at[0], wg, load_sem.at[3]),
        pltpu.make_async_copy(w_up.at[0], wu, load_sem.at[4]),
        pltpu.make_async_copy(w_down.at[0], wd, load_sem.at[5]),
    ]
    for copy in loads:
        copy.start()

    barrier = pltpu.get_barrier_semaphore()
    peers = [y_peer, edp_peer, ahead, behind]
    peers += [at(place(y, a, b + d, core)) for d in range(1, SIDE)]
    peers += [at(place(y, a, b + d, 1 - core)) for d in range(SIDE)]
    peers += [at(place(y, a + d, b, 1 - core)) for d in range(1, SIDE)]
    for peer in peers:
        pl.semaphore_signal(barrier, inc=1, device_id=peer, device_id_type=pl.DeviceIdType.MESH)

    experts = TARGETS * TARGETS
    names = lax.broadcasted_iota(jnp.int32, (experts, rows), 0)
    named = jnp.zeros((experts, rows), F32)
    weight = jnp.zeros((experts, rows), F32)
    for k in range(routes.shape[0]):
        match = names == routes[k : k + 1, :]
        named = named + jnp.where(match, 1.0, 0.0)
        weight = weight + jnp.where(match, gates[k : k + 1, :], 0.0)
    earlier = (
        lax.broadcasted_iota(jnp.int32, (rows, rows), 0)
        < lax.broadcasted_iota(jnp.int32, (rows, rows), 1)
    )
    earlier = jnp.where(earlier, 1.0, 0.0).astype(BF)
    count = dot(named.astype(BF), earlier)
    aux[0, 0, 0:experts, :] = jnp.where(named > 0.5, count, -1.0).astype(BF)
    aux[0, 0, experts : 2 * experts, :] = weight.astype(BF)
    hot[...] = jnp.zeros_like(hot)

    with jax.named_scope("barrier"):
        pl.semaphore_wait(barrier, len(peers))
        loads[0].wait()

    def remote(src, dst, send, receive, peer):
        return pltpu.make_async_remote_copy(
            src_ref=src, dst_ref=dst, send_sem=send, recv_sem=receive,
            device_id=peer, device_id_type=pl.DeviceIdType.MESH,
        )

    def half(dy):
        return pl.ds(rows * dy, rows)

    def columns(c):
        return pl.ds(c * (width // COLS), width // COLS)

    def token_copies(source, target, peer, send, receive, c):
        k, i = source
        m, j = target
        copies = [remote(blocks.at[k, half(i), columns(c)], blocks.at[m, half(j), columns(c)],
                         send.at[c], receive.at[c], peer)]
        if c == 0:
            copies.append(remote(aux.at[k, i], aux.at[m, j], send.at[COLS], receive.at[COLS], peer))
        return copies

    def y_copy(c):
        return token_copies(SEAT[0, 0], SEAT[0, 1], y_peer, y_s, y_r, c)

    def a_copy(slot, dy, c):
        source, peer = SEAT[0, dy], ahead if slot == 1 else behind
        if slot == 2 and dy == 0:
            source, peer = (SEAT[1, 0], ahead) if c == 0 else (SEAT[3, 0], behind)
        elif slot == 2:
            source, peer = SEAT[2, 0], y_peer
        return token_copies(source, SEAT[slot, dy], peer, a_s.at[2 * slot - 2 + dy],
                            a_r.at[2 * slot - 2 + dy], c)

    def begin(copies):
        for copy in copies:
            copy.start()

    def arrived(copies, name):
        with jax.named_scope(name):
            for copy in copies:
                copy.wait_recv()

    def a_start(slot, dy, c):
        begin(a_copy(slot, dy, c))

    def a_wait(slot, dy, c):
        arrived(a_copy(slot, dy, c), f"await{slot}{dy}{c}")

    e_copies = [
        remote(xs.at[0], xs.at[1], e_s.at[0], e_r.at[0], edp_peer),
        remote(ys.at[0], ys.at[1], e_s.at[1], e_r.at[1], edp_peer),
    ]

    def backward(r):
        def body(n):
            cols = tile(n)
            g = dot(xs[r], wg[:, cols])
            u = dot(xs[r], wu[:, cols])
            dh = dot(ys[r], wd[cols, :], ((1,), (1,)))
            s = jax.nn.sigmoid(g)
            act = g * s
            hid[r, :, cols] = (act * u).astype(BF)
            dgs[r, :, cols] = (dh * u * s * (1.0 + g * (1.0 - s))).astype(BF)
            dus[r, :, cols] = (dh * act).astype(BF)

        with jax.named_scope(f"bwd{r}"):
            loop(hidden_width // TILE, body)

    def fill_hot(d, weighted):
        slots = lax.broadcasted_iota(jnp.int32, (CAP, rows), 0).astype(F32)
        for dy in range(2):
            aux32[dy] = aux[d, dy].astype(F32)
        for t in range(TARGETS):
            e = forward_to(t)
            for dy in range(2):
                hit = aux32[dy, pl.ds(e, 1), :] == slots
                value = aux32[dy, pl.ds(e + experts, 1), :] if weighted else 1.0
                at_row = PAIR * t + CAP * dy
                hot[at_row : at_row + CAP, rows * dy : rows * dy + rows] = jnp.where(hit, value, 0.0)

    def b_copy(d, t):
        span = pl.ds(PAIR * t, PAIR)
        return remote(packed.at[d, span], recv.at[d, span], b_s.at[d], b_r.at[d], at(forward_to(t)))

    others = pl.ds(PAIR, CHUNK - PAIR)

    def b_all(d):
        return remote(packed.at[d, others], recv.at[d, others], b_s.at[d], b_r.at[d], y_peer)

    def group(q):
        return pl.ds(q * per_group * TILE, per_group * TILE)

    def rb_copy(d, t, q):
        span = pl.ds(PAIR * t, PAIR)
        return remote(recv.at[d, span, group(q)], back.at[d, span, group(q)], rb_s.at[q, d],
                      rb_r.at[q, d], at(forwarder(t)))

    def rb_all(d, q):
        return remote(recv.at[d, others, group(q)], back.at[d, others, group(q)], rb_s.at[q, d],
                      rb_r.at[q, d], y_peer)

    def pack(d):
        with jax.named_scope(f"pack{d}"):
            fill_hot(d, False)
            hot_lhs[...] = hot[...].astype(BF)

            def body(n):
                cols = tile(n)
                rows_out = dot(hot_lhs[...], blocks[d, :, cols]).astype(BF)
                packed[d, :, cols] = rows_out
                recv[d, 0:PAIR, cols] = rows_out[0:PAIR]

            loop(tiles, body)
            for t in (2, 6, 3, 7, 4, 5, 1):
                b_copy(d, t).start()

    def up(d):
        with jax.named_scope(f"upwait{d}"):
            b_all(d).wait_recv()

        def body(n):
            cols = tile(n)
            g = dot(recv[d], wg[:, cols])
            u = dot(recv[d], wu[:, cols])
            hbuf[d, :, cols] = (g * jax.nn.sigmoid(g) * u).astype(BF)

        with jax.named_scope(f"up{d}"):
            loop(hidden_width // TILE, body)

    def down(d, q):
        def body(n):
            cols = tile(n + q * per_group)
            out = dot(hbuf[d], wd[:, cols]).astype(BF)
            recv[d, :, cols] = out
            back[d, 0:PAIR, cols] = out[0:PAIR]

        with jax.named_scope(f"down{d}{q}"):
            loop(per_group, body)
            for t in (2, 3, 6, 7, 4, 5, 1):
                rb_copy(d, t, q).start()

    def mix(d):
        with jax.named_scope(f"mix{d}"):
            fill_hot(d, True)
            mix_lhs[d] = hot[...].T.astype(BF)

    def ra_copy(k, q):
        i = 1 if k in (0, 2) else 0
        dy = k // 2
        side = 0 if k in (0, 3) else 1
        return remote(part.at[k, half(i), group(q)], gathered.at[2 * dy + side, :, group(q)],
                      ra_s.at[k, q], ra_r.at[2 * dy + side, q], behind if side == 0 else ahead)

    def ra_wait(k, q):
        ra_copy(k, q).wait_recv()

    def low(q):
        return q < GROUPS // 2

    def rp_copy(k, q):
        peer = y_peer if k == 3 else (behind if low(q) else ahead)
        return remote(part.at[k, half(1), group(q)], passed.at[k // 2, :, group(q)],
                      rp_s.at[k // 2, q], rp_r.at[k // 2, q], peer)

    def ry_copy(q):
        return remote(y_send.at[:, group(q)], y_recv.at[:, group(q)], ry_s.at[q], ry_r.at[q], y_peer)

    def returned(k, q):
        with jax.named_scope(f"rbwait{k}{q}"):
            rb_all(k, q).wait_recv()

    def each_tile(q, body):
        loop(per_group, lambda n: body(tile(n + q * per_group)))

    def third(q):
        returned(3, q)

        def body(cols):
            part[3, :, cols] = dot(mix_lhs[3], back[3, :, cols]).astype(BF)

        with jax.named_scope(f"third{q}"):
            each_tile(q, body)
            rp_copy(3, q).start()
            ra_copy(3, q).start()

    def second(q):
        returned(2, q)

        def body(cols):
            value = dot(mix_lhs[2], back[2, :, cols])
            part[2, half(1), cols] = value[rows : 2 * rows].astype(BF)
            total[:, cols] = value[0:rows]

        with jax.named_scope(f"second{q}"):
            each_tile(q, body)
            ra_copy(2, q).start()

    def first(q):
        returned(1, q)
        arrived([rp_copy(3, q)], f"rpwait3{q}")

        def body(cols):
            value = dot(mix_lhs[1], back[1, :, cols])
            part[1, half(1), cols] = (value[rows : 2 * rows] + passed[1, :, cols].astype(F32)).astype(BF)
            if low(q):
                part[1, half(0), cols] = value[0:rows].astype(BF)

        with jax.named_scope(f"first{q}"):
            each_tile(q, body)
            rp_copy(1, q).start()
            if low(q):
                ra_copy(1, q).start()

    def first_late(q):
        arrived([rp_copy(1, q)], f"rpwait1{q}")

        def body(cols):
            value = dot(mix_lhs[1, half(0), :], back[1, :, cols])
            part[1, half(0), cols] = (value + passed[0, :, cols].astype(F32)).astype(BF)

        with jax.named_scope(f"firstlate{q}"):
            each_tile(q, body)
            ra_copy(1, q).start()

    def zeroth(q):
        returned(0, q)
        if low(q):
            arrived([rp_copy(1, q)], f"rpwait1{q}")

        def body(cols):
            value = dot(mix_lhs[0], back[0, :, cols])
            rest = value[rows : 2 * rows]
            if low(q):
                rest = rest + passed[0, :, cols].astype(F32)
            part[0, half(1), cols] = rest.astype(BF)
            total[:, cols] = value[0:rows]

        with jax.named_scope(f"zeroth{q}"):
            each_tile(q, body)
            ra_copy(0, q).start()

    def home(q):
        arrived([ra_copy(3, q), ra_copy(2, q)], f"rawait{q}")

        def body(cols):
            value = total[:, cols] + gathered[2, :, cols].astype(F32) + gathered[3, :, cols].astype(F32)
            y_send[:, cols] = value.astype(BF)

        with jax.named_scope(f"home{q}"):
            each_tile(q, body)
            ry_copy(q).start()

    def finish(q):
        arrived([ry_copy(q), ra_copy(1, q), ra_copy(0, q)], f"lastwait{q}")

        def body(cols):
            value = total[:, cols] + y_recv[:, cols].astype(F32)
            value = value + gathered[0, :, cols].astype(F32) + gathered[1, :, cols].astype(F32)
            mixed[:, cols] = value.astype(BF)

        each_tile(q, body)

    def in_weight_grads():
        def body(n):
            cols = pl.ds(pl.multiple_of(replica * half_width + n * TILE, TILE), TILE)
            for out, source in ((grad_gate, dgs), (grad_up, dus)):
                sums = [dot(xs[r, :, cols], source[r], ((0,), (0,))).astype(BF).astype(F32) for r in range(2)]
                out[0, tile(n), :] = sums[0] + sums[1]

        with jax.named_scope("gradin"):
            loop(half_width // TILE, body)

    def down_weight_grad():
        size = 512

        def body(n):
            own_cols = pl.ds(pl.multiple_of(replica * half_hidden, 128), half_hidden)
            sums = [
                dot(hid[r, :, own_cols], ys[r, :, tile(n, size)], ((0,), (0,))).astype(BF).astype(F32)
                for r in range(2)
            ]
            grad_down[0, :, tile(n, size)] = sums[0] + sums[1]

        with jax.named_scope("graddown"):
            loop(width // size, body)

    begin(y_copy(0))
    a_start(1, 0, 0)
    a_start(3, 0, 1)
    a_start(1, 0, 1)
    a_start(3, 0, 0)
    begin(y_copy(1))
    with jax.named_scope("wload"):
        for copy in loads[1:]:
            copy.wait()
    backward(0)
    a_wait(1, 0, 0)
    a_start(2, 0, 0)
    a_wait(3, 0, 1)
    a_start(2, 0, 1)
    arrived(y_copy(0), "ywait0")
    a_start(1, 1, 0)
    a_start(3, 1, 0)
    a_wait(1, 0, 1)
    pack(0)
    for c in range(COLS):
        a_wait(2, 0, c)
        a_start(2, 1, c)
    begin(e_copies)
    arrived(y_copy(1), "ywait1")
    a_start(1, 1, 1)
    a_start(3, 1, 1)
    a_wait(3, 0, 0)
    pack(1)
    for c in range(COLS):
        a_wait(3, 1, c)
    pack(2)
    for c in range(COLS):
        a_wait(1, 1, c)
        a_wait(2, 1, c)
    pack(3)
    up(0)
    mix(3)
    mix(2)
    up(1)
    mix(1)
    mix(0)
    up(2)
    for q in range(GROUPS):
        down(2, q)
    low_groups, high_groups = tuple(range(GROUPS // 2)), tuple(range(GROUPS // 2, GROUPS))
    up(3)
    for k in (3, 1, 0):
        for q in range(GROUPS):
            down(k, q)
    for q in range(GROUPS):
        third(q)
    for q in range(GROUPS):
        second(q)
    for pair in zip(high_groups, low_groups):
        for q in pair:
            first(q)
    arrived(e_copies, "ewait")
    backward(1)
    in_weight_grads()
    for q in range(GROUPS):
        home(q)
    for q, p in zip(high_groups, low_groups):
        zeroth(q)
        first_late(q)
        zeroth(p)
    down_weight_grad()
    with jax.named_scope("drain"):
        for copy in e_copies:
            copy.wait_send()
        for c in range(COLS):
            for copy in y_copy(c):
                copy.wait_send()
            for slot in range(1, SIDE):
                for dy in range(2):
                    for copy in a_copy(slot, dy, c):
                        copy.wait_send()
        for d in range(SIDE):
            b_all(d).wait_send()
        for q in range(GROUPS):
            for k in range(SIDE):
                rb_all(k, q).wait_send()
            for k in (1, 3):
                rp_copy(k, q).wait_send()
            for k in (2, 3):
                ra_copy(k, q).wait_send()
    for q, p in zip(high_groups, low_groups):
        finish(q)
        finish(p)
    with jax.named_scope("lastdrain"):
        for q in range(GROUPS):
            for k in (0, 1):
                ra_copy(k, q).wait_send()
            ry_copy(q).wait_send()


def flush(*refs):
    count = len(refs) // 2
    sems = refs[-1]
    copies = [
        pltpu.make_async_copy(source, target, sems.at[n])
        for n, (source, target) in enumerate(zip(refs[:count], refs[count : 2 * count]))
    ]
    for copy in copies:
        copy.start()
    for copy in copies:
        copy.wait()


def shards(tokens, routes, gate_weights, w_gate, w_up, w_down, saved_inputs, saved_cotangent):
    rows, width = tokens.shape
    hidden = w_gate.shape[2]
    back_rows = saved_inputs.shape[1]
    anywhere = pl.BlockSpec(memory_space=pl.ANY)
    whole = pl.BlockSpec(memory_space=pltpu.VMEM)
    dma = pltpu.SemaphoreType.DMA
    vm = pltpu.VMEM
    held = pl.pallas_call(
        kernel,
        out_shape=(
            pltpu.VMEM((rows, width), BF),
            pltpu.VMEM((1, width // 2, hidden), F32),
            pltpu.VMEM((1, width // 2, hidden), F32),
            pltpu.VMEM((1, hidden // 2, width), F32),
        ),
        in_specs=[whole, whole] + [anywhere] * 6,
        out_specs=(whole,) * 4,
        scratch_shapes=[
            vm((width, hidden), BF), vm((width, hidden), BF), vm((hidden, width), BF),
            vm((SIDE, 2 * rows, width), BF),
            vm((SIDE, 2, 128, rows), BF), vm((2, 128, rows), F32),
            vm((CHUNK, 2 * rows), F32), vm((CHUNK, 2 * rows), BF), vm((SIDE, 2 * rows, CHUNK), BF),
            vm((SIDE, CHUNK, width), BF), vm((SIDE, CHUNK, width), BF), vm((SIDE, CHUNK, width), BF),
            vm((SIDE, 2 * rows, width), BF), vm((SIDE, rows, width), BF), vm((2, rows, width), BF),
            vm((rows, width), BF), vm((rows, width), BF), vm((rows, width), F32),
            vm((2, back_rows, width), BF), vm((2, back_rows, width), BF),
            vm((2, back_rows, hidden), BF), vm((2, back_rows, hidden), BF), vm((2, back_rows, hidden), BF),
            vm((SIDE, CHUNK, hidden), BF),
            dma((6,)), dma((COLS + 1,)), dma((COLS + 1,)), dma((6, COLS + 1)), dma((6, COLS + 1)),
            dma((SIDE,)), dma((SIDE,)),
            dma((GROUPS, SIDE)), dma((GROUPS, SIDE)),
            dma((2, GROUPS)), dma((2, GROUPS)), dma((SIDE, GROUPS)), dma((SIDE, GROUPS)),
            dma((GROUPS,)), dma((GROUPS,)), dma((2,)), dma((2,)),
        ],
        compiler_params=pltpu.CompilerParams(
            collective_id=0, has_side_effects=True, vmem_limit_bytes=53 * 1024 * 1024
        ),
        cost_estimate=pl.CostEstimate(flops=22 * 10**9, bytes_accessed=40 * 10**6, transcendentals=2 * 10**6),
    )(routes.T, gate_weights.T, tokens, w_gate, w_up, w_down, saved_inputs, saved_cotangent)
    return pl.pallas_call(
        flush,
        out_shape=tuple(jax.ShapeDtypeStruct(h.shape, h.dtype) for h in held),
        in_specs=[anywhere] * 4,
        out_specs=(anywhere,) * 4,
        scratch_shapes=[dma((4,))],
        compiler_params=pltpu.CompilerParams(vmem_limit_bytes=1024 * 1024),
        cost_estimate=pl.CostEstimate(flops=0, bytes_accessed=20 * 10**6, transcendentals=0),
    )(*[pltpu.with_memory_space_constraint(h, pltpu.VMEM) for h in held])


def solution(mesh):
    return jax.shard_map(
        shards,
        mesh=mesh,
        in_specs=(
            P(("edp", "ep"), None),
            P(("edp", "ep"), None),
            P(("edp", "ep"), None),
            P("ep", None, None),
            P("ep", None, None),
            P("ep", None, None),
            P("ep", "edp", None),
            P("ep", "edp", None),
        ),
        out_specs=(
            P(("edp", "ep"), None),
            P("ep", "edp", None),
            P("ep", "edp", None),
            P("ep", "edp", None),
        ),
        check_vma=False,
    )
```

```python
import jax
import jax.numpy as jnp
from jax import lax
from jax.experimental import pallas as pl
from jax.experimental.pallas import tpu as pltpu
from jax.sharding import PartitionSpec as P

CAP = 24
SIDE = 4
TARGETS = 8
PAIR = 2 * CAP
CHUNK = TARGETS * PAIR
TILE = 256
GROUPS = 2
COLS = 2
SEAT = {(0, 0): (0, 0), (1, 0): (0, 1), (3, 0): (1, 0), (2, 0): (1, 1),
        (0, 1): (2, 0), (3, 1): (2, 1), (1, 1): (3, 0), (2, 1): (3, 1)}
BF = jnp.bfloat16
F32 = jnp.float32


def dot(a, b, dims=((1,), (0,))):
    return lax.dot_general(a, b, (dims, ((), ())), preferred_element_type=F32)


def tile(n, size=TILE):
    return pl.ds(pl.multiple_of(n * size, size), size)


def loop(count, body):
    def step(n, carry):
        body(n)
        return carry

    lax.fori_loop(0, count, step, 0)


def kernel(
    routes, gates, tokens, w_gate, w_up, w_down, saved_x, saved_y,
    mixed, grad_gate, grad_up, grad_down,
    wg, wu, wd, blocks, aux, aux32, hot, hot_lhs, mix_lhs, packed, recv, back, part, gathered, passed,
    y_send, y_recv, total, xs, ys, hid, dgs, dus, hbuf,
    load_sem, y_s, y_r, a_s, a_r, b_s, b_r, rb_s, rb_r, rp_s, rp_r, ra_s, ra_r, ry_s, ry_r, e_s, e_r,
):
    width = blocks.shape[-1]
    rows = blocks.shape[1] // 2
    hidden_width = wg.shape[1]
    half_width = width // 2
    half_hidden = hidden_width // 2
    tiles = width // TILE
    per_group = tiles // GROUPS

    me = lax.axis_index("ep")
    replica = lax.axis_index("edp")
    core = lax.rem(me, 2)
    x = lax.rem(me // 2, SIDE)
    z = lax.rem(me // (2 * SIDE), SIDE)
    y = me // (2 * SIDE * SIDE)
    a = z * (1 - core) + x * core
    b = x * (1 - core) + z * core

    def place(yy, aa, bb, cc):
        aa = lax.rem(aa, SIDE)
        bb = lax.rem(bb, SIDE)
        zz = aa * (1 - core) + bb * core
        xx = bb * (1 - core) + aa * core
        return ((yy * SIDE + zz) * SIDE + xx) * 2 + cc

    def at(index):
        return (replica, index)

    y_peer = at(place(1 - y, a, b, core))
    edp_peer = (1 - replica, me)
    ahead = at(place(y, a + 1, b, core))
    behind = at(place(y, a + SIDE - 1, b, core))

    def forward_to(t):
        f, g = t // 2, t % 2
        return place(y, a, b + f, core if g == 0 else 1 - core)

    def forwarder(t):
        f, g = t // 2, t % 2
        if g == 0:
            return place(y, a, b + SIDE - f, core)
        return place(y, a + SIDE - f, b, 1 - core)

    loads = [
        pltpu.make_async_copy(tokens, blocks.at[0, 0:rows], load_sem.at[0]),
        pltpu.make_async_copy(saved_x.at[0], xs.at[0], load_sem.at[1]),
        pltpu.make_async_copy(saved_y.at[0], ys.at[0], load_sem.at[2]),
        pltpu.make_async_copy(w_gate.at[0], wg, load_sem.at[3]),
        pltpu.make_async_copy(w_up.at[0], wu, load_sem.at[4]),
        pltpu.make_async_copy(w_down.at[0], wd, load_sem.at[5]),
    ]
    for copy in loads:
        copy.start()

    barrier = pltpu.get_barrier_semaphore()
    peers = [y_peer, edp_peer, ahead, behind]
    peers += [at(place(y, a, b + d, core)) for d in range(1, SIDE)]
    peers += [at(place(y, a, b + d, 1 - core)) for d in range(SIDE)]
    peers += [at(place(y, a + d, b, 1 - core)) for d in range(1, SIDE)]
    for peer in peers:
        pl.semaphore_signal(barrier, inc=1, device_id=peer, device_id_type=pl.DeviceIdType.MESH)

    experts = TARGETS * TARGETS
    names = lax.broadcasted_iota(jnp.int32, (experts, rows), 0)
    named = jnp.zeros((experts, rows), F32)
    weight = jnp.zeros((experts, rows), F32)
    for k in range(routes.shape[0]):
        match = names == routes[k : k + 1, :]
        named = named + jnp.where(match, 1.0, 0.0)
        weight = weight + jnp.where(match, gates[k : k + 1, :], 0.0)
    earlier = (
        lax.broadcasted_iota(jnp.int32, (rows, rows), 0)
        < lax.broadcasted_iota(jnp.int32, (rows, rows), 1)
    )
    earlier = jnp.where(earlier, 1.0, 0.0).astype(BF)
    count = dot(named.astype(BF), earlier)
    aux[0, 0, 0:experts, :] = jnp.where(named > 0.5, count, -1.0).astype(BF)
    aux[0, 0, experts : 2 * experts, :] = weight.astype(BF)
    hot[...] = jnp.zeros_like(hot)

    with jax.named_scope("barrier"):
        pl.semaphore_wait(barrier, len(peers))
        loads[0].wait()

    def remote(src, dst, send, receive, peer):
        return pltpu.make_async_remote_copy(
            src_ref=src, dst_ref=dst, send_sem=send, recv_sem=receive,
            device_id=peer, device_id_type=pl.DeviceIdType.MESH,
        )

    def half(dy):
        return pl.ds(rows * dy, rows)

    def columns(c):
        return pl.ds(c * (width // COLS), width // COLS)

    def token_copies(source, target, peer, send, receive, c):
        k, i = source
        m, j = target
        copies = [remote(blocks.at[k, half(i), columns(c)], blocks.at[m, half(j), columns(c)],
                         send.at[c], receive.at[c], peer)]
        if c == 0:
            copies.append(remote(aux.at[k, i], aux.at[m, j], send.at[COLS], receive.at[COLS], peer))
        return copies

    def y_copy(c):
        return token_copies(SEAT[0, 0], SEAT[0, 1], y_peer, y_s, y_r, c)

    def a_copy(slot, dy, c):
        source, peer = SEAT[0, dy], ahead if slot == 1 else behind
        if slot == 2 and dy == 0:
            source, peer = (SEAT[1, 0], ahead) if c == 0 else (SEAT[3, 0], behind)
        elif slot == 2:
            source, peer = SEAT[2, 0], y_peer
        return token_copies(source, SEAT[slot, dy], peer, a_s.at[2 * slot - 2 + dy],
                            a_r.at[2 * slot - 2 + dy], c)

    def begin(copies):
        for copy in copies:
            copy.start()

    def arrived(copies, name):
        with jax.named_scope(name):
            for copy in copies:
                copy.wait_recv()

    def a_start(slot, dy, c):
        begin(a_copy(slot, dy, c))

    def a_wait(slot, dy, c):
        arrived(a_copy(slot, dy, c), f"await{slot}{dy}{c}")

    e_copies = [
        remote(xs.at[0], xs.at[1], e_s.at[0], e_r.at[0], edp_peer),
        remote(ys.at[0], ys.at[1], e_s.at[1], e_r.at[1], edp_peer),
    ]

    def backward(r):
        def body(n):
            cols = tile(n)
            g = dot(xs[r], wg[:, cols])
            u = dot(xs[r], wu[:, cols])
            dh = dot(ys[r], wd[cols, :], ((1,), (1,)))
            s = jax.nn.sigmoid(g)
            act = g * s
            hid[r, :, cols] = (act * u).astype(BF)
            dgs[r, :, cols] = (dh * u * s * (1.0 + g * (1.0 - s))).astype(BF)
            dus[r, :, cols] = (dh * act).astype(BF)

        with jax.named_scope(f"bwd{r}"):
            loop(hidden_width // TILE, body)

    def fill_hot(d, weighted):
        slots = lax.broadcasted_iota(jnp.int32, (CAP, rows), 0).astype(F32)
        for dy in range(2):
            aux32[dy] = aux[d, dy].astype(F32)
        for t in range(TARGETS):
            e = forward_to(t)
            for dy in range(2):
                hit = aux32[dy, pl.ds(e, 1), :] == slots
                value = aux32[dy, pl.ds(e + experts, 1), :] if weighted else 1.0
                at_row = PAIR * t + CAP * dy
                hot[at_row : at_row + CAP, rows * dy : rows * dy + rows] = jnp.where(hit, value, 0.0)

    def b_copy(d, t):
        span = pl.ds(PAIR * t, PAIR)
        return remote(packed.at[d, span], recv.at[d, span], b_s.at[d], b_r.at[d], at(forward_to(t)))

    others = pl.ds(PAIR, CHUNK - PAIR)

    def b_all(d):
        return remote(packed.at[d, others], recv.at[d, others], b_s.at[d], b_r.at[d], y_peer)

    def group(q):
        return pl.ds(q * per_group * TILE, per_group * TILE)

    def rb_copy(d, t, q):
        span = pl.ds(PAIR * t, PAIR)
        return remote(recv.at[d, span, group(q)], back.at[d, span, group(q)], rb_s.at[q, d],
                      rb_r.at[q, d], at(forwarder(t)))

    def rb_all(d, q):
        return remote(recv.at[d, others, group(q)], back.at[d, others, group(q)], rb_s.at[q, d],
                      rb_r.at[q, d], y_peer)

    def pack(d):
        with jax.named_scope(f"pack{d}"):
            fill_hot(d, False)
            hot_lhs[...] = hot[...].astype(BF)

            def body(n):
                cols = tile(n)
                rows_out = dot(hot_lhs[...], blocks[d, :, cols]).astype(BF)
                packed[d, :, cols] = rows_out
                recv[d, 0:PAIR, cols] = rows_out[0:PAIR]

            loop(tiles, body)
            for t in (2, 6, 3, 7, 4, 5, 1):
                b_copy(d, t).start()

    def up(d):
        with jax.named_scope(f"upwait{d}"):
            b_all(d).wait_recv()

        def body(n):
            cols = tile(n)
            g = dot(recv[d], wg[:, cols])
            u = dot(recv[d], wu[:, cols])
            hbuf[d, :, cols] = (g * jax.nn.sigmoid(g) * u).astype(BF)

        with jax.named_scope(f"up{d}"):
            loop(hidden_width // TILE, body)

    def down(d, q):
        def body(n):
            cols = tile(n + q * per_group)
            out = dot(hbuf[d], wd[:, cols]).astype(BF)
            recv[d, :, cols] = out
            back[d, 0:PAIR, cols] = out[0:PAIR]

        with jax.named_scope(f"down{d}{q}"):
            loop(per_group, body)
            for t in (2, 3, 6, 7, 4, 5, 1):
                rb_copy(d, t, q).start()

    def mix(d):
        with jax.named_scope(f"mix{d}"):
            fill_hot(d, True)
            mix_lhs[d] = hot[...].T.astype(BF)

    def ra_copy(k, q):
        i = 1 if k in (0, 2) else 0
        dy = k // 2
        side = 0 if k in (0, 3) else 1
        return remote(part.at[k, half(i), group(q)], gathered.at[2 * dy + side, :, group(q)],
                      ra_s.at[k, q], ra_r.at[2 * dy + side, q], behind if side == 0 else ahead)

    def ra_wait(k, q):
        ra_copy(k, q).wait_recv()

    def low(q):
        return q < GROUPS // 2

    def rp_copy(k, q):
        peer = y_peer if k == 3 else (behind if low(q) else ahead)
        return remote(part.at[k, half(1), group(q)], passed.at[k // 2, :, group(q)],
                      rp_s.at[k // 2, q], rp_r.at[k // 2, q], peer)

    def ry_copy(q):
        return remote(y_send.at[:, group(q)], y_recv.at[:, group(q)], ry_s.at[q], ry_r.at[q], y_peer)

    def returned(k, q):
        with jax.named_scope(f"rbwait{k}{q}"):
            rb_all(k, q).wait_recv()

    def each_tile(q, body):
        loop(per_group, lambda n: body(tile(n + q * per_group)))

    def third(q):
        returned(3, q)

        def body(cols):
            part[3, :, cols] = dot(mix_lhs[3], back[3, :, cols]).astype(BF)

        with jax.named_scope(f"third{q}"):
            each_tile(q, body)
            rp_copy(3, q).start()
            ra_copy(3, q).start()

    def second(q):
        returned(2, q)

        def body(cols):
            value = dot(mix_lhs[2], back[2, :, cols])
            part[2, half(1), cols] = value[rows : 2 * rows].astype(BF)
            total[:, cols] = value[0:rows]

        with jax.named_scope(f"second{q}"):
            each_tile(q, body)
            ra_copy(2, q).start()

    def first(q):
        returned(1, q)
        arrived([rp_copy(3, q)], f"rpwait3{q}")

        def body(cols):
            value = dot(mix_lhs[1], back[1, :, cols])
            part[1, half(1), cols] = (value[rows : 2 * rows] + passed[1, :, cols].astype(F32)).astype(BF)
            if low(q):
                part[1, half(0), cols] = value[0:rows].astype(BF)

        with jax.named_scope(f"first{q}"):
            each_tile(q, body)
            rp_copy(1, q).start()
            if low(q):
                ra_copy(1, q).start()

    def first_late(q):
        arrived([rp_copy(1, q)], f"rpwait1{q}")

        def body(cols):
            value = dot(mix_lhs[1, half(0), :], back[1, :, cols])
            part[1, half(0), cols] = (value + passed[0, :, cols].astype(F32)).astype(BF)

        with jax.named_scope(f"firstlate{q}"):
            each_tile(q, body)
            ra_copy(1, q).start()

    def zeroth(q):
        returned(0, q)
        if low(q):
            arrived([rp_copy(1, q)], f"rpwait1{q}")

        def body(cols):
            value = dot(mix_lhs[0], back[0, :, cols])
            rest = value[rows : 2 * rows]
            if low(q):
                rest = rest + passed[0, :, cols].astype(F32)
            part[0, half(1), cols] = rest.astype(BF)
            total[:, cols] = value[0:rows]

        with jax.named_scope(f"zeroth{q}"):
            each_tile(q, body)
            ra_copy(0, q).start()

    def home(q):
        arrived([ra_copy(3, q), ra_copy(2, q)], f"rawait{q}")

        def body(cols):
            value = total[:, cols] + gathered[2, :, cols].astype(F32) + gathered[3, :, cols].astype(F32)
            y_send[:, cols] = value.astype(BF)

        with jax.named_scope(f"home{q}"):
            each_tile(q, body)
            ry_copy(q).start()

    def finish(q):
        arrived([ry_copy(q), ra_copy(1, q), ra_copy(0, q)], f"lastwait{q}")

        def body(cols):
            value = total[:, cols] + y_recv[:, cols].astype(F32)
            value = value + gathered[0, :, cols].astype(F32) + gathered[1, :, cols].astype(F32)
            mixed[:, cols] = value.astype(BF)

        each_tile(q, body)

    def in_weight_grads():
        def body(n):
            cols = pl.ds(pl.multiple_of(replica * half_width + n * TILE, TILE), TILE)
            for out, source in ((grad_gate, dgs), (grad_up, dus)):
                sums = [dot(xs[r, :, cols], source[r], ((0,), (0,))).astype(BF).astype(F32) for r in range(2)]
                out[0, tile(n), :] = sums[0] + sums[1]

        with jax.named_scope("gradin"):
            loop(half_width // TILE, body)

    def down_weight_grad():
        size = 512

        def body(n):
            own_cols = pl.ds(pl.multiple_of(replica * half_hidden, 128), half_hidden)
            sums = [
                dot(hid[r, :, own_cols], ys[r, :, tile(n, size)], ((0,), (0,))).astype(BF).astype(F32)
                for r in range(2)
            ]
            grad_down[0, :, tile(n, size)] = sums[0] + sums[1]

        with jax.named_scope("graddown"):
            loop(width // size, body)

    begin(y_copy(0))
    a_start(1, 0, 0)
    a_start(3, 0, 1)
    a_start(1, 0, 1)
    a_start(3, 0, 0)
    begin(y_copy(1))
    with jax.named_scope("wload"):
        for copy in loads[1:]:
            copy.wait()
    backward(0)
    a_wait(1, 0, 0)
    a_start(2, 0, 0)
    a_wait(3, 0, 1)
    a_start(2, 0, 1)
    arrived(y_copy(0), "ywait0")
    a_start(1, 1, 0)
    a_start(3, 1, 0)
    a_wait(1, 0, 1)
    pack(0)
    for c in range(COLS):
        a_wait(2, 0, c)
        a_start(2, 1, c)
    arrived(y_copy(1), "ywait1")
    a_start(1, 1, 1)
    a_start(3, 1, 1)
    a_wait(3, 0, 0)
    pack(1)
    begin(e_copies)
    for c in range(COLS):
        a_wait(3, 1, c)
    pack(2)
    for c in range(COLS):
        a_wait(1, 1, c)
        a_wait(2, 1, c)
    pack(3)
    up(0)
    mix(3)
    mix(2)
    up(1)
    mix(1)
    mix(0)
    up(2)
    for q in range(GROUPS):
        down(2, q)
    low_groups, high_groups = tuple(range(GROUPS // 2)), tuple(range(GROUPS // 2, GROUPS))
    up(3)
    for k in (3, 1, 0):
        for q in range(GROUPS):
            down(k, q)
    for q in range(GROUPS):
        third(q)
    for q in range(GROUPS):
        second(q)
    for pair in zip(high_groups, low_groups):
        for q in pair:
            first(q)
    arrived(e_copies, "ewait")
    backward(1)
    in_weight_grads()
    for q in range(GROUPS):
        home(q)
    for q, p in zip(high_groups, low_groups):
        zeroth(q)
        first_late(q)
        zeroth(p)
    down_weight_grad()
    with jax.named_scope("drain"):
        for copy in e_copies:
            copy.wait_send()
        for c in range(COLS):
            for copy in y_copy(c):
                copy.wait_send()
            for slot in range(1, SIDE):
                for dy in range(2):
                    for copy in a_copy(slot, dy, c):
                        copy.wait_send()
        for d in range(SIDE):
            b_all(d).wait_send()
        for q in range(GROUPS):
            for k in range(SIDE):
                rb_all(k, q).wait_send()
            for k in (1, 3):
                rp_copy(k, q).wait_send()
            for k in (2, 3):
                ra_copy(k, q).wait_send()
    for q, p in zip(high_groups, low_groups):
        finish(q)
        finish(p)
    with jax.named_scope("lastdrain"):
        for q in range(GROUPS):
            for k in (0, 1):
                ra_copy(k, q).wait_send()
            ry_copy(q).wait_send()


def flush(*refs):
    count = len(refs) // 2
    sems = refs[-1]
    copies = [
        pltpu.make_async_copy(source, target, sems.at[n])
        for n, (source, target) in enumerate(zip(refs[:count], refs[count : 2 * count]))
    ]
    for copy in copies:
        copy.start()
    for copy in copies:
        copy.wait()


def shards(tokens, routes, gate_weights, w_gate, w_up, w_down, saved_inputs, saved_cotangent):
    rows, width = tokens.shape
    hidden = w_gate.shape[2]
    back_rows = saved_inputs.shape[1]
    anywhere = pl.BlockSpec(memory_space=pl.ANY)
    whole = pl.BlockSpec(memory_space=pltpu.VMEM)
    dma = pltpu.SemaphoreType.DMA
    vm = pltpu.VMEM
    held = pl.pallas_call(
        kernel,
        out_shape=(
            pltpu.VMEM((rows, width), BF),
            pltpu.VMEM((1, width // 2, hidden), F32),
            pltpu.VMEM((1, width // 2, hidden), F32),
            pltpu.VMEM((1, hidden // 2, width), F32),
        ),
        in_specs=[whole, whole] + [anywhere] * 6,
        out_specs=(whole,) * 4,
        scratch_shapes=[
            vm((width, hidden), BF), vm((width, hidden), BF), vm((hidden, width), BF),
            vm((SIDE, 2 * rows, width), BF),
            vm((SIDE, 2, 128, rows), BF), vm((2, 128, rows), F32),
            vm((CHUNK, 2 * rows), F32), vm((CHUNK, 2 * rows), BF), vm((SIDE, 2 * rows, CHUNK), BF),
            vm((SIDE, CHUNK, width), BF), vm((SIDE, CHUNK, width), BF), vm((SIDE, CHUNK, width), BF),
            vm((SIDE, 2 * rows, width), BF), vm((SIDE, rows, width), BF), vm((2, rows, width), BF),
            vm((rows, width), BF), vm((rows, width), BF), vm((rows, width), F32),
            vm((2, back_rows, width), BF), vm((2, back_rows, width), BF),
            vm((2, back_rows, hidden), BF), vm((2, back_rows, hidden), BF), vm((2, back_rows, hidden), BF),
            vm((SIDE, CHUNK, hidden), BF),
            dma((6,)), dma((COLS + 1,)), dma((COLS + 1,)), dma((6, COLS + 1)), dma((6, COLS + 1)),
            dma((SIDE,)), dma((SIDE,)),
            dma((GROUPS, SIDE)), dma((GROUPS, SIDE)),
            dma((2, GROUPS)), dma((2, GROUPS)), dma((SIDE, GROUPS)), dma((SIDE, GROUPS)),
            dma((GROUPS,)), dma((GROUPS,)), dma((2,)), dma((2,)),
        ],
        compiler_params=pltpu.CompilerParams(
            collective_id=0, has_side_effects=True, vmem_limit_bytes=53 * 1024 * 1024
        ),
        cost_estimate=pl.CostEstimate(flops=22 * 10**9, bytes_accessed=40 * 10**6, transcendentals=2 * 10**6),
    )(routes.T, gate_weights.T, tokens, w_gate, w_up, w_down, saved_inputs, saved_cotangent)
    return pl.pallas_call(
        flush,
        out_shape=tuple(jax.ShapeDtypeStruct(h.shape, h.dtype) for h in held),
        in_specs=[anywhere] * 4,
        out_specs=(anywhere,) * 4,
        scratch_shapes=[dma((4,))],
        compiler_params=pltpu.CompilerParams(vmem_limit_bytes=1024 * 1024),
        cost_estimate=pl.CostEstimate(flops=0, bytes_accessed=20 * 10**6, transcendentals=0),
    )(*[pltpu.with_memory_space_constraint(h, pltpu.VMEM) for h in held])


def solution(mesh):
    return jax.shard_map(
        shards,
        mesh=mesh,
        in_specs=(
            P(("edp", "ep"), None),
            P(("edp", "ep"), None),
            P(("edp", "ep"), None),
            P("ep", None, None),
            P("ep", None, None),
            P("ep", None, None),
            P("ep", "edp", None),
            P("ep", "edp", None),
        ),
        out_specs=(
            P(("edp", "ep"), None),
            P("ep", "edp", None),
            P("ep", "edp", None),
            P("ep", "edp", None),
        ),
        check_vma=False,
    )
```
